8 devices in a mesh: sys: 1 (over z), aux: 2 (over y), orb: 4 (over x, core).
Axes of the slice: x: 2, y: 2, z: 1, core: 2. Of those that a mesh axis runs over, the one named last changes fastest.
Arguments:
- fit_tensor: float32 [1020, 348, 348], P(('sys', 'aux'), 'orb')
- occ_orbitals: float32 [348, 30], P('sys')
Outputs:
- output: float32 [348, 348], P(('sys', 'orb'), 'aux')
All inputs are finite; a program needn't handle non-finite values.
Results may differ from the reference program's by a relative error of at most 0.001.
Values are sent between devices in bfloat16 or wider.
A program may use at most 1 GiB of HBM per device.

```python
import math
import jax
import jax.numpy as jnp
from jax import lax

NBF = 348
NOCC = 30
NAUX = 1020

PREC_MODE = lax.Precision.HIGHEST


def setup_inputs(seed: int = 0, part: int = 0) -> dict:
    root_key = jax.random.fold_in(jax.random.key(seed), part)
    key_orb, key_dir, key_wgt, key_noise = jax.random.split(root_key, 4)
    orbitals = jnp.linalg.qr(jax.random.normal(key_orb, (NBF, NOCC), jnp.float32))[0]
    n_groups = 64
    directions = jax.random.normal(key_dir, (n_groups, NBF), jnp.float32)
    weights = jax.random.normal(key_wgt, (NAUX,), jnp.float32)
    group_of = jnp.arange(NAUX) * n_groups // NAUX
    noise_keys = jax.random.split(key_noise, NAUX)
    noise_scale = math.sqrt(math.sqrt(n_groups) / (NAUX * NOCC))

    def one_aux(packed):
        aux_key, weight, grp_index = packed
        noise_mat = jax.random.normal(aux_key, (NBF, NBF), jnp.float32)
        direction = directions[grp_index]
        sym_noise = (noise_mat + noise_mat.T) * math.sqrt(0.5)
        return noise_scale * (sym_noise + weight * jnp.outer(direction, direction))

    fit_tensor = lax.map(one_aux, (noise_keys, weights, group_of))
    return {'fit_tensor': fit_tensor, 'occ_orbitals': orbitals}


def reference(fit_tensor, occ_orbitals):
    density = jnp.dot(occ_orbitals, occ_orbitals.T, precision=PREC_MODE, preferred_element_type=jnp.float32)
    fit_flat = fit_tensor.reshape(NAUX, NBF * NBF)
    aux_coef = jnp.dot(fit_flat, density.reshape(NBF * NBF), precision=PREC_MODE, preferred_element_type=jnp.float32)
    coulomb = jnp.dot(aux_coef, fit_flat, precision=PREC_MODE, preferred_element_type=jnp.float32).reshape(NBF, NBF)
    half_t = jnp.dot(fit_tensor.reshape(NAUX * NBF, NBF), occ_orbitals, precision=PREC_MODE, preferred_element_type=jnp.float32).reshape(NAUX, NBF, NOCC)
    exchange = jnp.einsum('qmi,qni->mn', half_t, half_t, precision=PREC_MODE, preferred_element_type=jnp.float32)
    return 2.0 * coulomb - exchange
```

```python
import jax
import jax.numpy as jnp
from jax import lax
from jax.experimental import pallas as pl
from jax.experimental.pallas import tpu as pltpu
from jax.sharding import PartitionSpec as P

f32 = jnp.float32
bf16 = jnp.bfloat16

NOCC = 30
ROWS = 87
RPAD = 88
NBF = 348
NQ = 510
QT = 4
GRP = 8
NGRP = 11
RING = 3
EARLY = 4
ICH = 3
NCH = NOCC // ICH
HALF = 174


def pieces(x):
    hi = x.astype(bf16)
    rest = x - hi.astype(f32)
    mid = rest.astype(bf16)
    low = (rest - mid.astype(f32)).astype(bf16)
    return hi, mid, low


def pieces32(x):
    hi = x.astype(bf16).astype(f32)
    rest = x - hi
    mid = rest.astype(bf16).astype(f32)
    return hi, mid, rest - mid


def dot_nt(a, b):
    return lax.dot_general(a, b, (((1,), (1,)), ((), ())), preferred_element_type=f32)


def full_nt(a, b):
    n = a.shape[0]
    ah, am, al = pieces32(a)
    bh, bm, bl = pieces32(b)
    first = dot_nt(jnp.concatenate([ah, am, al], axis=0), bh)
    second = dot_nt(jnp.concatenate([ah, am], axis=0), bm)
    third = dot_nt(ah, bl)
    small = (first[2 * n:] + second[n:]) + third
    return first[:n] + ((first[n:2 * n] + second[:n]) + small)


def kernel(bt, ct, out, ring, tb, sb, rb, gacc, cst, cown, gown, grecv, jt, ks, kr, rsend, rrecv,
           pf, ph, dma_sem, d2d_s, d2d_r, ici_s, ici_r, g_s, g_r, r_s, r_r, p_s, p_r):
    y = lax.axis_index('aux')
    o = lax.axis_index('orb')
    p = o // 2
    s = lax.rem(o, 2)
    sib = o + 1 - 2 * s
    opp = lax.rem(o + 2, 4)
    opp_sib = 3 - o
    yo = 1 - y
    keep = 2 * p
    give = 2 * (1 - p)

    def dev(yy, oo):
        return {'aux': yy, 'orb': oo}

    def remote(src, dst, ssem, rsem, to):
        return pltpu.make_async_remote_copy(src_ref=src, dst_ref=dst, send_sem=ssem, recv_sem=rsem,
                                            device_id=to, device_id_type=pl.DeviceIdType.MESH)

    def load(step, j):
        m = lax.rem(step, NGRP) * GRP + j
        slot = lax.rem(step, RING) * GRP + j
        return m, pltpu.make_async_copy(bt.at[m], ring.at[slot], dma_sem.at[slot])

    def start_group(step):
        for j in range(GRP):
            m, copy = load(step, j)

            @pl.when(m < ROWS)
            def _():
                copy.start()

    def wait_group(step):
        for j in range(GRP):
            m, copy = load(step, j)

            @pl.when(m < ROWS)
            def _():
                copy.wait()

    for step in range(RING - 1):
        start_group(step)

    barrier = pltpu.get_barrier_semaphore()
    peers = [(y, sib), (y, opp), (y, opp_sib), (yo, o), (yo, sib), (yo, opp), (yo, opp_sib)]
    for peer in peers:
        pl.semaphore_signal(barrier, inc=1, device_id=dev(*peer), device_id_type=pl.DeviceIdType.MESH)
    pl.semaphore_wait(barrier, len(peers))

    t4 = tb.reshape(QT, NOCC, RPAD, 128)

    def early_copy(g):
        rows = pl.ds(pl.multiple_of(g * GRP, GRP), GRP)
        return remote(t4.at[pl.ds(give, 2), :, rows], rb.at[:, :, rows], ici_s.at[g], ici_r.at[g], dev(y, opp))

    def late_copy(c):
        orbs = pl.ds(c * ICH, ICH)
        rows = pl.ds(EARLY * GRP, RPAD - EARLY * GRP)
        return remote(t4.at[pl.ds(give, 2), orbs, rows], rb.at[:, orbs, rows],
                      ici_s.at[EARLY + c], ici_r.at[EARLY + c], dev(y, opp))

    def sib_copy(g):
        rows = pl.ds(pl.multiple_of(g * GRP, GRP), GRP)
        return remote(t4.at[:, :, rows], sb.at[:, :, rows], d2d_s.at[g], d2d_r.at[g], dev(y, sib))

    c = jnp.concatenate([ct[...], jnp.zeros((2, NBF), f32)], axis=0)
    cst[...] = jnp.concatenate(pieces(c), axis=0)
    mine = c[:, 0:ROWS]
    for b in range(1, 4):
        mine = jnp.where(o == b, c[:, b * ROWS:(b + 1) * ROWS], mine)
    cown[...] = jnp.concatenate([mine, jnp.zeros((32, 128 - ROWS), f32)], axis=1)
    gacc[...] = jnp.zeros_like(gacc)
    jt[...] = jnp.zeros_like(jt)
    ks[...] = jnp.zeros_like(ks)
    kr[...] = jnp.zeros_like(kr)

    def t_step(g, carry):
        start_group(g + RING - 1)
        wait_group(g)
        cg = pltpu.roll(cown[...], lax.rem(128 - g * GRP, 128), 1)
        for j in range(GRP):
            m = g * GRP + j
            x = ring[lax.rem(g, RING) * GRP + j]
            r = None
            for piece in pieces(x):
                term = jnp.dot(cst[...], piece, preferred_element_type=f32)
                r = term if r is None else r + term
            t = r[0:32] + r[32:64] + r[64:96]
            if j == GRP - 1:
                t = jnp.where(m < ROWS, t, 0.0)
            gacc[:, 0:NQ] += t * cg[:, j:j + 1]
            for k in range(QT):
                hi = min(NQ, 128 * (k + 1))
                tt = t[:NOCC, 128 * k:hi]
                if hi < 128 * (k + 1):
                    tt = jnp.concatenate([tt, jnp.zeros((NOCC, 128 * (k + 1) - hi), f32)], axis=1)
                tb[k, pl.ds(m, NOCC, stride=RPAD), :] = tt
        sib_copy(g).start()

        @pl.when(g < EARLY)
        def _():
            early_copy(g).start()
        return carry

    lax.fori_loop(0, NGRP, t_step, 0)

    gown[...] = jnp.sum(gacc[...], axis=0, keepdims=True)
    g_copies = [remote(gown, grecv.at[k], g_s.at[k], g_r.at[k], dev(y, to))
                for k, to in enumerate((sib, opp, opp_sib))]
    for copy in g_copies:
        copy.start()

    def late_start(c, carry):
        late_copy(c).start()
        return carry

    lax.fori_loop(0, NCH, late_start, 0)

    def sib_wait(g, carry):
        sib_copy(g).wait_recv()
        return carry

    lax.fori_loop(0, NGRP, sib_wait, 0)

    def both(tiles_own, tiles_sib):
        own = jnp.concatenate(tiles_own, axis=1)
        other = jnp.concatenate(tiles_sib, axis=1)
        gap = jnp.zeros((128 - RPAD, own.shape[1]), f32)
        return own, jnp.concatenate([own, gap, other], axis=0)

    def k_self(i):
        own, stack = both([t4[k, i] for k in range(QT)], [sb[k, i] for k in range(QT)])
        res = full_nt(own, stack)
        ks[:, 0:128 + RPAD] += res

    def self_step(i, carry):
        k_self(i)
        return carry

    ahead = NOCC - 2 * NGRP
    lax.fori_loop(0, ahead, self_step, 0)

    for copy in g_copies:
        copy.wait()
    gam = gown[...] + grecv[0] + grecv[1] + grecv[2]
    gown[...] = gam
    lane = lax.broadcasted_iota(jnp.int32, (NBF, 128), 1)

    def j_step(g, carry):
        step = g + NGRP

        @pl.when(step + RING - 1 < 2 * NGRP)
        def _():
            start_group(step + RING - 1)
        wait_group(step)
        gv = gown[:, 0:NQ]
        acc = jt[...]
        for j in range(GRP):
            x = ring[lax.rem(step, RING) * GRP + j]
            col = jnp.sum(x * gv, axis=1, keepdims=True)
            acc = jnp.where(lane == g * GRP + j, col, acc)
        jt[...] = acc
        k_self(ahead + 2 * g)
        k_self(ahead + 2 * g + 1)
        return carry

    lax.fori_loop(0, NGRP, j_step, 0)

    lane88 = lax.broadcasted_iota(jnp.int32, (RPAD, 128), 1)

    def columns(first, second):
        a = jnp.where(s == 0, first, second)
        b = pltpu.roll(jnp.where(s == 0, second, first), ROWS, 1)
        return jnp.concatenate([jnp.where(lane88 < ROWS, a, b), b], axis=1)[:, 0:HALF]

    jrows = jnp.transpose(jt[...])[0:RPAD]
    j0 = 2.0 * jrows[:, 0:HALF]
    j1 = 2.0 * jrows[:, HALF:2 * HALF]
    kself = columns(ks[:, 0:128], ks[:, 128:256])
    h0 = j0 - jnp.where(p == 0, kself, 0.0)
    h1 = j1 - jnp.where(p == 1, kself, 0.0)
    rsend[:, 0:HALF] = jnp.where(y == 0, h1, h0)
    base = jnp.where(y == 0, h0, h1)
    ks[:, 0:HALF] = base
    r_copy = remote(rsend, rrecv, r_s, r_r, dev(yo, o))
    r_copy.start()

    def early_wait(g, carry):
        early_copy(g).wait_recv()
        return carry

    lax.fori_loop(0, EARLY, early_wait, 0)

    def r_step(c, carry):
        late_copy(c).wait_recv()
        for di in range(ICH):
            i = c * ICH + di
            _, stack = both([t4[keep + k, i] for k in range(2)], [sb[keep + k, i] for k in range(2)])
            moved = jnp.concatenate([rb[k, i] for k in range(2)], axis=1)
            kr[:, 0:128 + RPAD] += full_nt(moved, stack)
        return carry

    lax.fori_loop(0, NCH, r_step, 0)

    p_full0 = remote(kr, pf.at[0], p_s.at[0], p_r.at[0], dev(y, opp))
    p_full1 = remote(kr, pf.at[1], p_s.at[0], p_r.at[1], dev(yo, opp))
    p_own = remote(kr.at[:, pl.ds(0, 128)], ph.at[0], p_s.at[1], p_r.at[2], dev(yo, o))
    p_sib0 = remote(kr.at[:, pl.ds(128, 128)], ph.at[1], p_s.at[2], p_r.at[3], dev(y, sib))
    p_sib1 = remote(kr.at[:, pl.ds(128, 128)], ph.at[2], p_s.at[2], p_r.at[4], dev(yo, sib))

    @pl.when(y == p)
    def _():
        for copy in (p_full0, p_sib1, p_own):
            copy.start()
        r_copy.wait()
        out[...] = (ks[:, 0:HALF] + rrecv[:, 0:HALF])[0:ROWS]
        for copy in (p_full0, p_sib1, p_own):
            copy.wait_send()

    @pl.when(y != p)
    def _():
        p_full1.start()
        p_sib0.start()
        r_copy.wait()
        for copy in (p_sib0, p_own, p_sib1):
            copy.wait_recv()
        col_opp = jnp.transpose(jnp.concatenate([kr[:, 0:128] + ph[0], jnp.zeros((40, 128), f32)], axis=0))[0:RPAD]
        col_sib = jnp.transpose(jnp.concatenate([ph[1] + ph[2], jnp.zeros((40, 128), f32)], axis=0))[0:RPAD]
        for copy in (p_full0, p_full1):
            copy.wait_recv()
        block_a = (pf[0, :, 0:128] + pf[1, :, 0:128]) + col_opp
        block_b = (pf[0, :, 128:256] + pf[1, :, 128:256]) + col_sib
        res = (ks[:, 0:HALF] + rrecv[:, 0:HALF]) - columns(block_a, block_b)
        out[...] = res[0:ROWS]
        p_full1.wait_send()
        p_sib0.wait_send()

    def sends_done(g, carry):
        sib_copy(g).wait_send()
        return carry

    lax.fori_loop(0, NGRP, sends_done, 0)

    def early_done(g, carry):
        early_copy(g).wait_send()
        return carry

    lax.fori_loop(0, EARLY, early_done, 0)

    def late_done(c, carry):
        late_copy(c).wait_send()
        return carry

    lax.fori_loop(0, NCH, late_done, 0)


def solution(mesh):
    sem = pltpu.SemaphoreType.DMA

    def local_fock(fit_loc, orbitals):
        bt = jnp.transpose(fit_loc, (1, 2, 0))
        ct = jnp.transpose(orbitals)
        return pl.pallas_call(
            kernel,
            out_shape=jax.ShapeDtypeStruct((ROWS, HALF), f32),
            in_specs=[pl.BlockSpec(memory_space=pl.ANY), pl.BlockSpec(memory_space=pltpu.VMEM)],
            out_specs=pl.BlockSpec(memory_space=pltpu.VMEM),
            scratch_shapes=[
                pltpu.VMEM((RING * GRP, NBF, NQ), f32),
                pltpu.VMEM((QT, NOCC * RPAD, 128), f32),
                pltpu.VMEM((QT, NOCC, RPAD, 128), f32),
                pltpu.VMEM((2, NOCC, RPAD, 128), f32),
                pltpu.VMEM((32, 512), f32),
                pltpu.VMEM((96, NBF), bf16),
                pltpu.VMEM((32, 128), f32),
                pltpu.VMEM((1, 512), f32),
                pltpu.VMEM((3, 1, 512), f32),
                pltpu.VMEM((NBF, 128), f32),
                pltpu.VMEM((RPAD, 256), f32),
                pltpu.VMEM((RPAD, 256), f32),
                pltpu.VMEM((RPAD, 256), f32),
                pltpu.VMEM((RPAD, 256), f32),
                pltpu.VMEM((2, RPAD, 256), f32),
                pltpu.VMEM((3, RPAD, 128), f32),
                sem((RING * GRP,)), sem((NGRP,)), sem((NGRP,)), sem((EARLY + NCH,)), sem((EARLY + NCH,)),
                sem((3,)), sem((3,)), sem, sem, sem((3,)), sem((5,)),
            ],
            compiler_params=pltpu.CompilerParams(collective_id=0, has_side_effects=True,
                                                 vmem_limit_bytes=60 << 20),
            name='fock',
        )(bt, ct)

    spec_fit = P(('sys', 'aux'), 'orb', None)
    spec_orbitals = P('sys', None)
    spec_out = P(('sys', 'orb'), 'aux')
    return jax.shard_map(local_fock, mesh=mesh, in_specs=(spec_fit, spec_orbitals), out_specs=spec_out, check_vma=False)
```

```python
import jax
import jax.numpy as jnp
from jax import lax
from jax.experimental import pallas as pl
from jax.experimental.pallas import tpu as pltpu
from jax.sharding import PartitionSpec as P

f32 = jnp.float32
bf16 = jnp.bfloat16

NOCC = 30
ROWS = 87
RPAD = 88
NBF = 348
NQ = 510
QT = 4
GRP = 8
NGRP = 11
RING = 3
EARLY = 5
FIRST = 2
ICH = 3
NCH = NOCC // ICH
HALF = 174


def pieces(x):
    hi = x.astype(bf16)
    rest = x - hi.astype(f32)
    mid = rest.astype(bf16)
    low = (rest - mid.astype(f32)).astype(bf16)
    return hi, mid, low


def pieces32(x):
    hi = x.astype(bf16).astype(f32)
    rest = x - hi
    mid = rest.astype(bf16).astype(f32)
    return hi, mid, rest - mid


def dot_nt(a, b):
    return lax.dot_general(a, b, (((1,), (1,)), ((), ())), preferred_element_type=f32)


def full_nt(a, b):
    n = a.shape[0]
    ah, am, al = pieces32(a)
    bh, bm, bl = pieces32(b)
    first = dot_nt(jnp.concatenate([ah, am, al], axis=0), bh)
    second = dot_nt(jnp.concatenate([ah, am], axis=0), bm)
    third = dot_nt(ah, bl)
    small = (first[2 * n:] + second[n:]) + third
    return first[:n] + ((first[n:2 * n] + second[:n]) + small)


def kernel(bt, ct_hbm, out, ring, ct, fb, e0, tb, sb, rb, gacc, cst, cown, gown, grecv, jt, ks, kr, rsend, rrecv,
           pf, ph, dma_sem, ct_sem, fb_sem, e_s, e_r, d2d_s, d2d_r, ici_s, ici_r, g_s, g_r, r_s, r_r, p_s, p_r):
    y = lax.axis_index('aux')
    o = lax.axis_index('orb')
    p = o // 2
    s = lax.rem(o, 2)
    sib = o + 1 - 2 * s
    opp = lax.rem(o + 2, 4)
    opp_sib = 3 - o
    yo = 1 - y
    keep = 2 * p
    give = 2 * (1 - p)

    def dev(yy, oo):
        return {'aux': yy, 'orb': oo}

    def remote(src, dst, ssem, rsem, to):
        return pltpu.make_async_remote_copy(src_ref=src, dst_ref=dst, send_sem=ssem, recv_sem=rsem,
                                            device_id=to, device_id_type=pl.DeviceIdType.MESH)

    def load(step, j):
        m = lax.rem(step, NGRP) * GRP + j
        slot = lax.rem(step, RING) * GRP + j
        return m, pltpu.make_async_copy(bt.at[m], ring.at[slot], dma_sem.at[slot])

    def start_group(step):
        for j in range(GRP):
            m, copy = load(step, j)

            @pl.when(m < ROWS)
            def _():
                copy.start()

    def wait_group(step):
        for j in range(GRP):
            m, copy = load(step, j)

            @pl.when(m < ROWS)
            def _():
                copy.wait()

    def first_load(m):
        lanes = pl.ds(pl.multiple_of(give * 128, 128), 128)
        return pltpu.make_async_copy(bt.at[m, :, lanes], fb.at[m], fb_sem.at[m])

    ct_copy = pltpu.make_async_copy(ct_hbm, ct, ct_sem)
    ct_copy.start()
    for m in range(FIRST * GRP):
        first_load(m).start()
    for step in range(RING - 1):
        start_group(step)

    barrier = pltpu.get_barrier_semaphore()
    peers = [(y, sib), (y, opp), (y, opp_sib), (yo, o), (yo, sib), (yo, opp), (yo, opp_sib)]
    for peer in peers:
        pl.semaphore_signal(barrier, inc=1, device_id=dev(*peer), device_id_type=pl.DeviceIdType.MESH)

    t4 = tb.reshape(QT, NOCC, RPAD, 128)

    def early_copy(g):
        rows = pl.ds(pl.multiple_of(g * GRP, GRP), GRP)
        return remote(t4.at[pl.ds(give, 2), :, rows], rb.at[:, :, rows], ici_s.at[g], ici_r.at[g], dev(y, opp))

    def early_rest(g):
        rows = pl.ds(pl.multiple_of(g * GRP, GRP), GRP)
        return remote(t4.at[pl.ds(give + 1, 1), :, rows], rb.at[pl.ds(1, 1), :, rows], ici_s.at[g], ici_r.at[g],
                      dev(y, opp))

    e4 = e0.reshape(FIRST, NOCC, GRP, 128)

    def first_copy(g):
        rows = pl.ds(g * GRP, GRP)
        return remote(e4.at[g], rb.at[0, :, rows], e_s.at[g], e_r.at[g], dev(y, opp))

    def late_copy(c):
        orbs = pl.ds(c * ICH, ICH)
        rows = pl.ds(EARLY * GRP, RPAD - EARLY * GRP)
        return remote(t4.at[pl.ds(give, 2), orbs, rows], rb.at[:, orbs, rows],
                      ici_s.at[EARLY + c], ici_r.at[EARLY + c], dev(y, opp))

    def sib_copy(g):
        rows = pl.ds(pl.multiple_of(g * GRP, GRP), GRP)
        return remote(t4.at[:, :, rows], sb.at[:, :, rows], d2d_s.at[g], d2d_r.at[g], dev(y, sib))

    ct_copy.wait()
    c = jnp.concatenate([ct[...], jnp.zeros((2, NBF), f32)], axis=0)
    cst[...] = jnp.concatenate(pieces(c), axis=0)
    mine = c[:, 0:ROWS]
    for b in range(1, 4):
        mine = jnp.where(o == b, c[:, b * ROWS:(b + 1) * ROWS], mine)
    cown[...] = jnp.concatenate([mine, jnp.zeros((32, 128 - ROWS), f32)], axis=1)
    gacc[...] = jnp.zeros_like(gacc)
    jt[...] = jnp.zeros_like(jt)
    ks[...] = jnp.zeros_like(ks)
    kr[...] = jnp.zeros_like(kr)

    def t_rows(x):
        r = None
        for piece in pieces(x):
            term = jnp.dot(cst[...], piece, preferred_element_type=f32)
            r = term if r is None else r + term
        return r[0:32] + r[32:64] + r[64:96]

    for g in range(FIRST):
        for j in range(GRP):
            first_load(g * GRP + j).wait()
        for j in range(GRP):
            e0[pl.ds(g * NOCC * GRP + j, NOCC, stride=GRP), :] = t_rows(fb[g * GRP + j])[:NOCC]
        if g == 0:
            pl.semaphore_wait(barrier, len(peers))
        first_copy(g).start()

    def t_step(g, carry):
        start_group(g + RING - 1)
        wait_group(g)
        cg = pltpu.roll(cown[...], lax.rem(128 - g * GRP, 128), 1)
        for j in range(GRP):
            m = g * GRP + j
            x = ring[lax.rem(g, RING) * GRP + j]
            t = t_rows(x)
            if j == GRP - 1:
                t = jnp.where(m < ROWS, t, 0.0)
            gacc[:, 0:NQ] += t * cg[:, j:j + 1]
            for k in range(QT):
                hi = min(NQ, 128 * (k + 1))
                tt = t[:NOCC, 128 * k:hi]
                if hi < 128 * (k + 1):
                    tt = jnp.concatenate([tt, jnp.zeros((NOCC, 128 * (k + 1) - hi), f32)], axis=1)
                tb[k, pl.ds(m, NOCC, stride=RPAD), :] = tt
        sib_copy(g).start()

        @pl.when(g < FIRST)
        def _():
            early_rest(g).start()

        @pl.when((g >= FIRST) & (g < EARLY))
        def _():
            early_copy(g).start()
        return carry

    lax.fori_loop(0, NGRP, t_step, 0)

    gown[...] = jnp.sum(gacc[...], axis=0, keepdims=True)
    g_copies = [remote(gown, grecv.at[k], g_s.at[k], g_r.at[k], dev(y, to))
                for k, to in enumerate((sib, opp, opp_sib))]
    for copy in g_copies:
        copy.start()

    def late_start(c, carry):
        late_copy(c).start()
        return carry

    lax.fori_loop(0, NCH, late_start, 0)

    def sib_wait(g, carry):
        sib_copy(g).wait_recv()
        return carry

    lax.fori_loop(0, NGRP, sib_wait, 0)

    def both(tiles_own, tiles_sib):
        own = jnp.concatenate(tiles_own, axis=1)
        other = jnp.concatenate(tiles_sib, axis=1)
        gap = jnp.zeros((128 - RPAD, own.shape[1]), f32)
        return own, jnp.concatenate([own, gap, other], axis=0)

    def k_self(i):
        own, stack = both([t4[k, i] for k in range(QT)], [sb[k, i] for k in range(QT)])
        res = full_nt(own, stack)
        ks[:, 0:128 + RPAD] += res

    def self_step(i, carry):
        k_self(i)
        return carry

    ahead = NOCC - 2 * NGRP
    lax.fori_loop(0, ahead, self_step, 0)

    for copy in g_copies:
        copy.wait()
    gam = gown[...] + grecv[0] + grecv[1] + grecv[2]
    gown[...] = gam
    lane = lax.broadcasted_iota(jnp.int32, (NBF, 128), 1)

    def j_step(g, carry):
        step = g + NGRP

        @pl.when(step + RING - 1 < 2 * NGRP)
        def _():
            start_group(step + RING - 1)
        wait_group(step)
        gv = gown[:, 0:NQ]
        acc = jt[...]
        for j in range(GRP):
            x = ring[lax.rem(step, RING) * GRP + j]
            col = jnp.sum(x * gv, axis=1, keepdims=True)
            acc = jnp.where(lane == g * GRP + j, col, acc)
        jt[...] = acc
        k_self(ahead + 2 * g)
        k_self(ahead + 2 * g + 1)
        return carry

    lax.fori_loop(0, NGRP, j_step, 0)

    lane88 = lax.broadcasted_iota(jnp.int32, (RPAD, 128), 1)

    def columns(first, second):
        a = jnp.where(s == 0, first, second)
        b = pltpu.roll(jnp.where(s == 0, second, first), ROWS, 1)
        return jnp.concatenate([jnp.where(lane88 < ROWS, a, b), b], axis=1)[:, 0:HALF]

    jrows = jnp.transpose(jt[...])[0:RPAD]
    j0 = 2.0 * jrows[:, 0:HALF]
    j1 = 2.0 * jrows[:, HALF:2 * HALF]
    kself = columns(ks[:, 0:128], ks[:, 128:256])
    h0 = j0 - jnp.where(p == 0, kself, 0.0)
    h1 = j1 - jnp.where(p == 1, kself, 0.0)
    rsend[:, 0:HALF] = jnp.where(y == 0, h1, h0)
    base = jnp.where(y == 0, h0, h1)
    ks[:, 0:HALF] = base
    r_copy = remote(rsend, rrecv, r_s, r_r, dev(yo, o))
    r_copy.start()

    def early_wait(g, carry):
        early_copy(g).wait_recv()
        return carry

    for g in range(FIRST):
        first_copy(g).wait_recv()
        early_rest(g).wait_recv()
    lax.fori_loop(FIRST, EARLY, early_wait, 0)

    def r_step(c, carry):
        late_copy(c).wait_recv()
        for di in range(ICH):
            i = c * ICH + di
            _, stack = both([t4[keep + k, i] for k in range(2)], [sb[keep + k, i] for k in range(2)])
            moved = jnp.concatenate([rb[k, i] for k in range(2)], axis=1)
            kr[:, 0:128 + RPAD] += full_nt(moved, stack)
        return carry

    lax.fori_loop(0, NCH, r_step, 0)

    p_full0 = remote(kr, pf.at[0], p_s.at[0], p_r.at[0], dev(y, opp))
    p_full1 = remote(kr, pf.at[1], p_s.at[0], p_r.at[1], dev(yo, opp))
    p_own = remote(kr.at[:, pl.ds(0, 128)], ph.at[0], p_s.at[1], p_r.at[2], dev(yo, o))
    p_sib0 = remote(kr.at[:, pl.ds(128, 128)], ph.at[1], p_s.at[2], p_r.at[3], dev(y, sib))
    p_sib1 = remote(kr.at[:, pl.ds(128, 128)], ph.at[2], p_s.at[2], p_r.at[4], dev(yo, sib))

    @pl.when(y == p)
    def _():
        for copy in (p_full0, p_sib1, p_own):
            copy.start()
        r_copy.wait()
        out[...] = (ks[:, 0:HALF] + rrecv[:, 0:HALF])[0:ROWS]
        for copy in (p_full0, p_sib1, p_own):
            copy.wait_send()

    @pl.when(y != p)
    def _():
        p_full1.start()
        p_sib0.start()
        r_copy.wait()
        for copy in (p_sib0, p_own, p_sib1):
            copy.wait_recv()
        col_opp = jnp.transpose(jnp.concatenate([kr[:, 0:128] + ph[0], jnp.zeros((40, 128), f32)], axis=0))[0:RPAD]
        col_sib = jnp.transpose(jnp.concatenate([ph[1] + ph[2], jnp.zeros((40, 128), f32)], axis=0))[0:RPAD]
        for copy in (p_full0, p_full1):
            copy.wait_recv()
        block_a = (pf[0, :, 0:128] + pf[1, :, 0:128]) + col_opp
        block_b = (pf[0, :, 128:256] + pf[1, :, 128:256]) + col_sib
        res = (ks[:, 0:HALF] + rrecv[:, 0:HALF]) - columns(block_a, block_b)
        out[...] = res[0:ROWS]
        p_full1.wait_send()
        p_sib0.wait_send()

    def sends_done(g, carry):
        sib_copy(g).wait_send()
        return carry

    lax.fori_loop(0, NGRP, sends_done, 0)

    def early_done(g, carry):
        early_copy(g).wait_send()
        return carry

    for g in range(FIRST):
        first_copy(g).wait_send()
        early_rest(g).wait_send()
    lax.fori_loop(FIRST, EARLY, early_done, 0)

    def late_done(c, carry):
        late_copy(c).wait_send()
        return carry

    lax.fori_loop(0, NCH, late_done, 0)


def solution(mesh):
    sem = pltpu.SemaphoreType.DMA

    def local_fock(fit_loc, orbitals):
        bt = jnp.transpose(fit_loc, (1, 2, 0))
        ct = jnp.transpose(orbitals)
        return pl.pallas_call(
            kernel,
            out_shape=pltpu.VMEM((ROWS, HALF), f32),
            in_specs=[pl.BlockSpec(memory_space=pl.ANY), pl.BlockSpec(memory_space=pl.ANY)],
            out_specs=pl.BlockSpec(memory_space=pltpu.VMEM),
            scratch_shapes=[
                pltpu.VMEM((RING * GRP, NBF, NQ), f32),
                pltpu.VMEM((NOCC, NBF), f32),
                pltpu.VMEM((FIRST * GRP, NBF, 128), f32),
                pltpu.VMEM((FIRST * NOCC * GRP, 128), f32),
                pltpu.VMEM((QT, NOCC * RPAD, 128), f32),
                pltpu.VMEM((QT, NOCC, RPAD, 128), f32),
                pltpu.VMEM((2, NOCC, RPAD, 128), f32),
                pltpu.VMEM((32, 512), f32),
                pltpu.VMEM((96, NBF), bf16),
                pltpu.VMEM((32, 128), f32),
                pltpu.VMEM((1, 512), f32),
                pltpu.VMEM((3, 1, 512), f32),
                pltpu.VMEM((NBF, 128), f32),
                pltpu.VMEM((RPAD, 256), f32),
                pltpu.VMEM((RPAD, 256), f32),
                pltpu.VMEM((RPAD, 256), f32),
                pltpu.VMEM((RPAD, 256), f32),
                pltpu.VMEM((2, RPAD, 256), f32),
                pltpu.VMEM((3, RPAD, 128), f32),
                sem((RING * GRP,)), sem, sem((FIRST * GRP,)), sem((FIRST,)), sem((FIRST,)), sem((NGRP,)), sem((NGRP,)), sem((EARLY + NCH,)), sem((EARLY + NCH,)),
                sem((3,)), sem((3,)), sem, sem, sem((3,)), sem((5,)),
            ],
            compiler_params=pltpu.CompilerParams(collective_id=0, has_side_effects=True,
                                                 vmem_limit_bytes=60 << 20),
            name='fock',
        )(bt, ct)

    spec_fit = P(('sys', 'aux'), 'orb', None)
    spec_orbitals = P('sys', None)
    spec_out = P(('sys', 'orb'), 'aux')
    return jax.shard_map(local_fock, mesh=mesh, in_specs=(spec_fit, spec_orbitals), out_specs=spec_out, check_vma=False)
```

```python
import jax
import jax.numpy as jnp
from jax import lax
from jax.experimental import pallas as pl
from jax.experimental.pallas import tpu as pltpu
from jax.sharding import PartitionSpec as P

f32 = jnp.float32
bf16 = jnp.bfloat16

NOCC = 30
ROWS = 87
RPAD = 88
NBF = 348
NQ = 510
QT = 4
GRP = 8
NGRP = 11
RING = 7
AHEAD = 2
AGAIN = NGRP - RING
EARLY = 6
FIRST = 2
ICH = 3
NCH = NOCC // ICH
HALF = 174


def pieces(x):
    hi = x.astype(bf16)
    rest = x - hi.astype(f32)
    mid = rest.astype(bf16)
    low = (rest - mid.astype(f32)).astype(bf16)
    return hi, mid, low


def pieces32(x):
    hi = x.astype(bf16).astype(f32)
    rest = x - hi
    mid = rest.astype(bf16).astype(f32)
    return hi, mid, rest - mid


def dot_nt(a, b):
    return lax.dot_general(a, b, (((1,), (1,)), ((), ())), preferred_element_type=f32)


def full_nt(a, b):
    n = a.shape[0]
    ah, am, al = pieces32(a)
    bh, bm, bl = pieces32(b)
    first = dot_nt(jnp.concatenate([ah, am, al], axis=0), bh)
    second = dot_nt(jnp.concatenate([ah, am], axis=0), bm)
    third = dot_nt(ah, bl)
    small = (first[2 * n:] + second[n:]) + third
    return first[:n] + ((first[n:2 * n] + second[:n]) + small)


def kernel(bt, ct_hbm, out, ring, ct, fb, e0, tb, sb, rb, gacc, cst, cown, gown, grecv, jt, ks, kr, rsend, rrecv,
           pf, ph, dma_sem, ct_sem, fb_sem, e_s, e_r, d2d_s, d2d_r, ici_s, ici_r, g_s, g_r, r_s, r_r, p_s, p_r):
    y = lax.axis_index('aux')
    o = lax.axis_index('orb')
    p = o // 2
    s = lax.rem(o, 2)
    sib = o + 1 - 2 * s
    opp = lax.rem(o + 2, 4)
    opp_sib = 3 - o
    yo = 1 - y
    keep = 2 * p
    give = 2 * (1 - p)

    def dev(yy, oo):
        return {'aux': yy, 'orb': oo}

    def remote(src, dst, ssem, rsem, to):
        return pltpu.make_async_remote_copy(src_ref=src, dst_ref=dst, send_sem=ssem, recv_sem=rsem,
                                            device_id=to, device_id_type=pl.DeviceIdType.MESH)

    def load(g, slot, j):
        m = g * GRP + j
        slot = slot * GRP + j
        return m, pltpu.make_async_copy(bt.at[m], ring.at[slot], dma_sem.at[slot])

    def start_group(g, slot):
        for j in range(GRP):
            m, copy = load(g, slot, j)

            @pl.when(m < ROWS)
            def _():
                copy.start(priority=1)

    def wait_group(g, slot):
        for j in range(GRP):
            m, copy = load(g, slot, j)

            @pl.when(m < ROWS)
            def _():
                copy.wait()

    def first_load(m):
        lanes = pl.ds(pl.multiple_of(give * 128, 128), 128)
        return pltpu.make_async_copy(bt.at[m, :, lanes], fb.at[m], fb_sem.at[m])

    ct_copy = pltpu.make_async_copy(ct_hbm, ct, ct_sem)
    ct_copy.start()
    for m in range(FIRST * GRP):
        first_load(m).start()
    for g in range(AHEAD):
        start_group(g, g)

    barrier = pltpu.get_barrier_semaphore()
    peers = [(y, sib), (y, opp), (y, opp_sib), (yo, o), (yo, sib), (yo, opp), (yo, opp_sib)]
    for peer in peers:
        pl.semaphore_signal(barrier, inc=1, device_id=dev(*peer), device_id_type=pl.DeviceIdType.MESH)

    t4 = tb.reshape(QT, NOCC, RPAD, 128)

    def early_copy(g):
        rows = pl.ds(pl.multiple_of(g * GRP, GRP), GRP)
        return remote(t4.at[pl.ds(give, 2), :, rows], rb.at[:, :, rows], ici_s.at[g], ici_r.at[g], dev(y, opp))

    def early_rest(g):
        rows = pl.ds(pl.multiple_of(g * GRP, GRP), GRP)
        return remote(t4.at[pl.ds(give + 1, 1), :, rows], rb.at[pl.ds(1, 1), :, rows], ici_s.at[g], ici_r.at[g],
                      dev(y, opp))

    e4 = e0.reshape(FIRST, NOCC, GRP, 128)

    def first_copy(g):
        rows = pl.ds(g * GRP, GRP)
        return remote(e4.at[g], rb.at[0, :, rows], e_s.at[g], e_r.at[g], dev(y, opp))

    def late_copy(c):
        orbs = pl.ds(c * ICH, ICH)
        rows = pl.ds(EARLY * GRP, RPAD - EARLY * GRP)
        return remote(t4.at[pl.ds(give, 2), orbs, rows], rb.at[:, orbs, rows],
                      ici_s.at[EARLY + c], ici_r.at[EARLY + c], dev(y, opp))

    def sib_copy(g):
        rows = pl.ds(pl.multiple_of(g * GRP, GRP), GRP)
        return remote(t4.at[:, :, rows], sb.at[:, :, rows], d2d_s.at[g], d2d_r.at[g], dev(y, sib))

    ct_copy.wait()
    c = jnp.concatenate([ct[...], jnp.zeros((2, NBF), f32)], axis=0)
    cst[...] = jnp.concatenate(pieces(c), axis=0)
    mine = c[:, 0:ROWS]
    for b in range(1, 4):
        mine = jnp.where(o == b, c[:, b * ROWS:(b + 1) * ROWS], mine)
    cown[...] = jnp.concatenate([mine, jnp.zeros((32, 128 - ROWS), f32)], axis=1)
    gacc[...] = jnp.zeros_like(gacc)
    jt[...] = jnp.zeros_like(jt)
    ks[...] = jnp.zeros_like(ks)
    kr[...] = jnp.zeros_like(kr)

    def t_rows(x):
        r = None
        for piece in pieces(x):
            term = jnp.dot(cst[...], piece, preferred_element_type=f32)
            r = term if r is None else r + term
        return r[0:32] + r[32:64] + r[64:96]

    for g in range(FIRST):
        for j in range(GRP):
            first_load(g * GRP + j).wait()
        for j in range(GRP):
            e0[pl.ds(g * NOCC * GRP + j, NOCC, stride=GRP), :] = t_rows(fb[g * GRP + j])[:NOCC]
        if g == 0:
            pl.semaphore_wait(barrier, len(peers))
        first_copy(g).start()

    def t_step(g, carry):
        slot = lax.rem(g, RING)

        @pl.when(g + AHEAD < NGRP)
        def _():
            start_group(g + AHEAD, lax.rem(g + AHEAD, RING))
        wait_group(g, slot)
        cg = pltpu.roll(cown[...], lax.rem(128 - g * GRP, 128), 1)
        for j in range(GRP):
            m = g * GRP + j
            x = ring[slot * GRP + j]
            t = t_rows(x)
            if j == GRP - 1:
                t = jnp.where(m < ROWS, t, 0.0)
            gacc[:, 0:NQ] += t * cg[:, j:j + 1]
            for k in range(QT):
                hi = min(NQ, 128 * (k + 1))
                tt = t[:NOCC, 128 * k:hi]
                if hi < 128 * (k + 1):
                    tt = jnp.concatenate([tt, jnp.zeros((NOCC, 128 * (k + 1) - hi), f32)], axis=1)
                tb[k, pl.ds(m, NOCC, stride=RPAD), :] = tt
        sib_copy(g).start()

        @pl.when(g < FIRST)
        def _():
            early_rest(g).start()

        @pl.when((g >= FIRST) & (g < EARLY))
        def _():
            early_copy(g).start()
        return carry

    lax.fori_loop(0, NGRP, t_step, 0)

    gown[...] = jnp.sum(gacc[...], axis=0, keepdims=True)
    g_copies = [remote(gown, grecv.at[k], g_s.at[k], g_r.at[k], dev(y, to))
                for k, to in enumerate((sib, opp, opp_sib))]
    for copy in g_copies:
        copy.start()

    def late_start(c, carry):
        late_copy(c).start()
        return carry

    lax.fori_loop(0, NCH, late_start, 0)

    def sib_wait(g, carry):
        sib_copy(g).wait_recv()
        return carry

    lax.fori_loop(0, NGRP, sib_wait, 0)

    def both(tiles_own, tiles_sib):
        own = jnp.concatenate(tiles_own, axis=1)
        other = jnp.concatenate(tiles_sib, axis=1)
        gap = jnp.zeros((128 - RPAD, own.shape[1]), f32)
        return own, jnp.concatenate([own, gap, other], axis=0)

    def k_self(i):
        own, stack = both([t4[k, i] for k in range(QT)], [sb[k, i] for k in range(QT)])
        res = full_nt(own, stack)
        ks[:, 0:128 + RPAD] += res

    def self_step(i, carry):
        k_self(i)
        return carry

    ahead = NOCC - 2 * NGRP
    lax.fori_loop(0, ahead, self_step, 0)

    for copy in g_copies:
        copy.wait()
    gam = gown[...] + grecv[0] + grecv[1] + grecv[2]
    gown[...] = gam
    lane = lax.broadcasted_iota(jnp.int32, (NBF, 128), 1)

    def j_step(n, carry):
        g = lax.rem(n + AGAIN, NGRP)
        slot = lax.rem(n + AGAIN, RING)

        @pl.when((n >= 1) & (n <= AGAIN))
        def _():
            start_group(n - 1, lax.rem(n - 1 + AGAIN, RING))

        @pl.when(n >= RING)
        def _():
            wait_group(g, slot)
        gv = gown[:, 0:NQ]
        acc = jt[...]
        for j in range(GRP):
            x = ring[slot * GRP + j]
            col = jnp.sum(x * gv, axis=1, keepdims=True)
            acc = jnp.where(lane == g * GRP + j, col, acc)
        jt[...] = acc
        k_self(ahead + 2 * n)
        k_self(ahead + 2 * n + 1)
        return carry

    lax.fori_loop(0, NGRP, j_step, 0)

    lane88 = lax.broadcasted_iota(jnp.int32, (RPAD, 128), 1)

    def columns(first, second):
        a = jnp.where(s == 0, first, second)
        b = pltpu.roll(jnp.where(s == 0, second, first), ROWS, 1)
        return jnp.concatenate([jnp.where(lane88 < ROWS, a, b), b], axis=1)[:, 0:HALF]

    jrows = jnp.transpose(jt[...])[0:RPAD]
    j0 = 2.0 * jrows[:, 0:HALF]
    j1 = 2.0 * jrows[:, HALF:2 * HALF]
    kself = columns(ks[:, 0:128], ks[:, 128:256])
    h0 = j0 - jnp.where(p == 0, kself, 0.0)
    h1 = j1 - jnp.where(p == 1, kself, 0.0)
    rsend[:, 0:HALF] = jnp.where(y == 0, h1, h0)
    base = jnp.where(y == 0, h0, h1)
    ks[:, 0:HALF] = base
    r_copy = remote(rsend, rrecv, r_s, r_r, dev(yo, o))
    r_copy.start()

    def early_wait(g, carry):
        early_copy(g).wait_recv()
        return carry

    for g in range(FIRST):
        first_copy(g).wait_recv()
        early_rest(g).wait_recv()
    lax.fori_loop(FIRST, EARLY, early_wait, 0)

    def r_step(c, carry):
        late_copy(c).wait_recv()
        for di in range(ICH):
            i = c * ICH + di
            _, stack = both([t4[keep + k, i] for k in range(2)], [sb[keep + k, i] for k in range(2)])
            moved = jnp.concatenate([rb[k, i] for k in range(2)], axis=1)
            kr[:, 0:128 + RPAD] += full_nt(moved, stack)
        return carry

    lax.fori_loop(0, NCH, r_step, 0)

    p_full0 = remote(kr, pf.at[0], p_s.at[0], p_r.at[0], dev(y, opp))
    p_full1 = remote(kr, pf.at[1], p_s.at[0], p_r.at[1], dev(yo, opp))
    p_own = remote(kr.at[:, pl.ds(0, 128)], ph.at[0], p_s.at[1], p_r.at[2], dev(yo, o))
    p_sib0 = remote(kr.at[:, pl.ds(128, 128)], ph.at[1], p_s.at[2], p_r.at[3], dev(y, sib))
    p_sib1 = remote(kr.at[:, pl.ds(128, 128)], ph.at[2], p_s.at[2], p_r.at[4], dev(yo, sib))

    @pl.when(y == p)
    def _():
        for copy in (p_full0, p_sib1, p_own):
            copy.start()
        r_copy.wait()
        out[...] = (ks[:, 0:HALF] + rrecv[:, 0:HALF])[0:ROWS]
        for copy in (p_full0, p_sib1, p_own):
            copy.wait_send()

    @pl.when(y != p)
    def _():
        p_full1.start()
        p_sib0.start()
        r_copy.wait()
        for copy in (p_sib0, p_own, p_sib1):
            copy.wait_recv()
        col_opp = jnp.transpose(jnp.concatenate([kr[:, 0:128] + ph[0], jnp.zeros((40, 128), f32)], axis=0))[0:RPAD]
        col_sib = jnp.transpose(jnp.concatenate([ph[1] + ph[2], jnp.zeros((40, 128), f32)], axis=0))[0:RPAD]
        for copy in (p_full0, p_full1):
            copy.wait_recv()
        block_a = (pf[0, :, 0:128] + pf[1, :, 0:128]) + col_opp
        block_b = (pf[0, :, 128:256] + pf[1, :, 128:256]) + col_sib
        res = (ks[:, 0:HALF] + rrecv[:, 0:HALF]) - columns(block_a, block_b)
        out[...] = res[0:ROWS]
        p_full1.wait_send()
        p_sib0.wait_send()

    def sends_done(g, carry):
        sib_copy(g).wait_send()
        return carry

    lax.fori_loop(0, NGRP, sends_done, 0)

    def early_done(g, carry):
        early_copy(g).wait_send()
        return carry

    for g in range(FIRST):
        first_copy(g).wait_send()
        early_rest(g).wait_send()
    lax.fori_loop(FIRST, EARLY, early_done, 0)

    def late_done(c, carry):
        late_copy(c).wait_send()
        return carry

    lax.fori_loop(0, NCH, late_done, 0)


def solution(mesh):
    sem = pltpu.SemaphoreType.DMA

    def local_fock(fit_loc, orbitals):
        bt = jnp.transpose(fit_loc, (1, 2, 0))
        ct = jnp.transpose(orbitals)
        return pl.pallas_call(
            kernel,
            out_shape=pltpu.VMEM((ROWS, HALF), f32),
            in_specs=[pl.BlockSpec(memory_space=pl.ANY), pl.BlockSpec(memory_space=pl.ANY)],
            out_specs=pl.BlockSpec(memory_space=pltpu.VMEM),
            scratch_shapes=[
                pltpu.VMEM((RING * GRP, NBF, NQ), f32),
                pltpu.VMEM((NOCC, NBF), f32),
                pltpu.VMEM((FIRST * GRP, NBF, 128), f32),
                pltpu.VMEM((FIRST * NOCC * GRP, 128), f32),
                pltpu.VMEM((QT, NOCC * RPAD, 128), f32),
                pltpu.VMEM((QT, NOCC, RPAD, 128), f32),
                pltpu.VMEM((2, NOCC, RPAD, 128), f32),
                pltpu.VMEM((32, 512), f32),
                pltpu.VMEM((96, NBF), bf16),
                pltpu.VMEM((32, 128), f32),
                pltpu.VMEM((1, 512), f32),
                pltpu.VMEM((3, 1, 512), f32),
                pltpu.VMEM((NBF, 128), f32),
                pltpu.VMEM((RPAD, 256), f32),
                pltpu.VMEM((RPAD, 256), f32),
                pltpu.VMEM((RPAD, 256), f32),
                pltpu.VMEM((RPAD, 256), f32),
                pltpu.VMEM((2, RPAD, 256), f32),
                pltpu.VMEM((3, RPAD, 128), f32),
                sem((RING * GRP,)), sem, sem((FIRST * GRP,)), sem((FIRST,)), sem((FIRST,)), sem((NGRP,)), sem((NGRP,)), sem((EARLY + NCH,)), sem((EARLY + NCH,)),
                sem((3,)), sem((3,)), sem, sem, sem((3,)), sem((5,)),
            ],
            compiler_params=pltpu.CompilerParams(collective_id=0, has_side_effects=True,
                                                 vmem_limit_bytes=63 << 20),
            name='fock',
        )(bt, ct)

    spec_fit = P(('sys', 'aux'), 'orb', None)
    spec_orbitals = P('sys', None)
    spec_out = P(('sys', 'orb'), 'aux')
    return jax.shard_map(local_fock, mesh=mesh, in_specs=(spec_fit, spec_orbitals), out_specs=spec_out, check_vma=False)
```

```python
import jax
import jax.numpy as jnp
from jax import lax
from jax.experimental import pallas as pl
from jax.experimental.pallas import tpu as pltpu
from jax.sharding import PartitionSpec as P

f32 = jnp.float32
bf16 = jnp.bfloat16

NOCC = 30
ROWS = 87
RPAD = 88
NBF = 348
NQ = 510
QT = 4
GRP = 8
NGRP = 11
RING = 7
AHEAD = 2
AGAIN = NGRP - RING
EARLY = 6
FIRST = 2
ICH = 3
NCH = NOCC // ICH
MAIN = RPAD - GRP
TAIL = ROWS - MAIN
DENSE = 216
CUTS = (0, 3, 6, 9, 12, 15, 18, 21, 24, 27, 30)
HALF = 174


def pieces(x):
    hi = x.astype(bf16)
    rest = x - hi.astype(f32)
    mid = rest.astype(bf16)
    low = (rest - mid.astype(f32)).astype(bf16)
    return hi, mid, low


def pieces32(x):
    hi = x.astype(bf16).astype(f32)
    rest = x - hi
    mid = rest.astype(bf16).astype(f32)
    return hi, mid, rest - mid


def dot_nt(a, b):
    return lax.dot_general(a, b, (((1,), (1,)), ((), ())), preferred_element_type=f32)


def full_nt(a, b):
    n = a.shape[0]
    ah, am, al = pieces32(a)
    bh, bm, bl = pieces32(b)
    first = dot_nt(jnp.concatenate([ah, am, al], axis=0), bh)
    second = dot_nt(jnp.concatenate([ah, am], axis=0), bm)
    third = dot_nt(ah, bl)
    small = (first[2 * n:] + second[n:]) + third
    return first[:n] + ((first[n:2 * n] + second[:n]) + small)


def kernel(bt, ct_hbm, out, ring, ct, fb, e0, tb, sb, rb, lt, rl, gacc, cst, cown, gown, grecv, jt, ks, kr, kl, rsend, rrecv,
           pf, ph, dma_sem, ct_sem, fb_sem, e_s, e_r, d2d_s, d2d_r, ici_s, ici_r, last_s, last_r, g_s, g_r, r_s, r_r, p_s, p_r):
    y = lax.axis_index('aux')
    o = lax.axis_index('orb')
    p = o // 2
    s = lax.rem(o, 2)
    sib = o + 1 - 2 * s
    opp = lax.rem(o + 2, 4)
    opp_sib = 3 - o
    yo = 1 - y
    keep = 2 * p
    give = 2 * (1 - p)

    def dev(yy, oo):
        return {'aux': yy, 'orb': oo}

    def remote(src, dst, ssem, rsem, to):
        return pltpu.make_async_remote_copy(src_ref=src, dst_ref=dst, send_sem=ssem, recv_sem=rsem,
                                            device_id=to, device_id_type=pl.DeviceIdType.MESH)

    def load(g, slot, j):
        m = g * GRP + j
        slot = slot * GRP + j
        return m, pltpu.make_async_copy(bt.at[m], ring.at[slot], dma_sem.at[slot])

    def start_group(g, slot):
        for j in range(GRP):
            m, copy = load(g, slot, j)

            @pl.when(m < ROWS)
            def _():
                copy.start(priority=1)

    def wait_group(g, slot):
        for j in range(GRP):
            m, copy = load(g, slot, j)

            @pl.when(m < ROWS)
            def _():
                copy.wait()

    def first_load(g):
        lanes = pl.ds(pl.multiple_of(give * 128, 128), 128)
        rows = pl.ds(g * GRP, GRP)
        return pltpu.make_async_copy(bt.at[rows, :, lanes], fb.at[rows], fb_sem.at[g])

    ct_copy = pltpu.make_async_copy(ct_hbm, ct, ct_sem)
    ct_copy.start()
    first_load(0).start()
    for g in range(AHEAD):
        start_group(g, g)

    barrier = pltpu.get_barrier_semaphore()
    peers = [(y, sib), (y, opp), (y, opp_sib), (yo, o), (yo, sib), (yo, opp), (yo, opp_sib)]
    for peer in peers:
        pl.semaphore_signal(barrier, inc=1, device_id=dev(*peer), device_id_type=pl.DeviceIdType.MESH)

    t4 = tb.reshape(QT, NOCC, RPAD, 128)

    def early_copy(g):
        rows = pl.ds(pl.multiple_of(g * GRP, GRP), GRP)
        return remote(t4.at[pl.ds(give, 2), :, rows], rb.at[:, :, rows], ici_s.at[g], ici_r.at[g], dev(y, opp))

    def early_rest(g):
        rows = pl.ds(pl.multiple_of(g * GRP, GRP), GRP)
        return remote(t4.at[pl.ds(give + 1, 1), :, rows], rb.at[pl.ds(1, 1), :, rows], ici_s.at[g], ici_r.at[g],
                      dev(y, opp))

    e4 = e0.reshape(FIRST, NOCC, GRP, 128)

    def first_copy(g):
        rows = pl.ds(g * GRP, GRP)
        return remote(e4.at[g], rb.at[0, :, rows], e_s.at[g], e_r.at[g], dev(y, opp))

    def late_copy(c):
        orbs = pl.ds(c * ICH, ICH)
        rows = pl.ds(EARLY * GRP, MAIN - EARLY * GRP)
        return remote(t4.at[pl.ds(give, 2), orbs, rows], rb.at[:, orbs, rows],
                      ici_s.at[EARLY + c], ici_r.at[EARLY + c], dev(y, opp))

    def last_copy(c):
        lo, hi = (-(-TAIL * CUTS[k] // GRP) * GRP for k in (c, c + 1))
        rows = pl.ds(lo, hi - lo)
        return remote(lt.at[pl.ds(give, 2), rows], rl.at[:, rows], last_s.at[c], last_r.at[c], dev(y, opp))

    def sib_copy(g):
        rows = pl.ds(pl.multiple_of(g * GRP, GRP), GRP)
        return remote(t4.at[:, :, rows], sb.at[:, :, rows], d2d_s.at[g], d2d_r.at[g], dev(y, sib))

    ct_copy.wait()
    c = jnp.concatenate([ct[...], jnp.zeros((2, NBF), f32)], axis=0)
    cst[...] = jnp.concatenate(pieces(c), axis=0)
    def t_rows(x):
        r = None
        for piece in pieces(x):
            term = jnp.dot(cst[...], piece, preferred_element_type=f32)
            r = term if r is None else r + term
        return r[0:32] + r[32:64] + r[64:96]

    for g in range(FIRST):
        first_load(g).wait()
        if g + 1 < FIRST:
            first_load(g + 1).start()
        for j in range(GRP):
            e0[pl.ds(g * NOCC * GRP + j, NOCC, stride=GRP), :] = t_rows(fb[g * GRP + j])[:NOCC]
        if g == 0:
            pl.semaphore_wait(barrier, len(peers))
        first_copy(g).start()

    mine = c[:, 0:ROWS]
    for b in range(1, 4):
        mine = jnp.where(o == b, c[:, b * ROWS:(b + 1) * ROWS], mine)
    cown[...] = jnp.concatenate([mine, jnp.zeros((32, 128 - ROWS), f32)], axis=1)
    gacc[...] = jnp.zeros_like(gacc)
    jt[...] = jnp.zeros_like(jt)
    ks[...] = jnp.zeros_like(ks)
    kr[...] = jnp.zeros_like(kr)
    kl[...] = jnp.zeros_like(kl)

    def t_group(g, rows, dense):
        slot = lax.rem(g, RING)
        if not dense:
            @pl.when(g + AHEAD < NGRP)
            def _():
                start_group(g + AHEAD, lax.rem(g + AHEAD, RING))
        wait_group(g, slot)
        cg = pltpu.roll(cown[...], lax.rem(128 - g * GRP, 128), 1)
        for j in range(rows):
            m = g * GRP + j
            t = t_rows(ring[slot * GRP + j])
            gacc[:, 0:NQ] += t * cg[:, j:j + 1]
            for k in range(QT):
                hi = min(NQ, 128 * (k + 1))
                tt = t[:NOCC, 128 * k:hi]
                if hi < 128 * (k + 1):
                    tt = jnp.concatenate([tt, jnp.zeros((NOCC, 128 * (k + 1) - hi), f32)], axis=1)
                tb[k, pl.ds(m, NOCC, stride=RPAD), :] = tt
                if dense:
                    lt[k, pl.ds(j, NOCC, stride=TAIL), :] = tt
        sib_copy(g).start()

    def t_step(g, carry):
        t_group(g, GRP, False)

        @pl.when(g < FIRST)
        def _():
            early_rest(g).start()

        @pl.when((g >= FIRST) & (g < EARLY))
        def _():
            early_copy(g).start()
        return carry

    lax.fori_loop(0, NGRP - 1, t_step, 0)
    for k in range(QT):
        tb[k, pl.ds(ROWS, NOCC, stride=RPAD), :] = jnp.zeros((NOCC, 128), f32)
        lt[k, DENSE - GRP:, :] = jnp.zeros((GRP, 128), f32)
    t_group(NGRP - 1, TAIL, True)

    gown[...] = jnp.sum(gacc[...], axis=0, keepdims=True)
    g_copies = [remote(gown, grecv.at[k], g_s.at[k], g_r.at[k], dev(y, to))
                for k, to in enumerate((sib, opp, opp_sib))]
    for copy in g_copies:
        copy.start()

    def late_start(c, carry):
        late_copy(c).start()
        return carry

    lax.fori_loop(0, NCH, late_start, 0)

    for c in range(len(CUTS) - 1):
        last_copy(c).start()

    def sib_wait(g, carry):
        sib_copy(g).wait_recv()
        return carry

    lax.fori_loop(0, NGRP, sib_wait, 0)

    def both(tiles_own, tiles_sib):
        own = jnp.concatenate(tiles_own, axis=1)
        other = jnp.concatenate(tiles_sib, axis=1)
        gap = jnp.zeros((128 - RPAD, own.shape[1]), f32)
        return own, jnp.concatenate([own, gap, other], axis=0)

    def k_self(i):
        own, stack = both([t4[k, i] for k in range(QT)], [sb[k, i] for k in range(QT)])
        res = full_nt(own, stack)
        ks[:, 0:128 + RPAD] += res

    def self_step(i, carry):
        k_self(i)
        return carry

    ahead = NOCC - 2 * NGRP
    lax.fori_loop(0, ahead, self_step, 0)

    for copy in g_copies:
        copy.wait()
    gam = gown[...] + grecv[0] + grecv[1] + grecv[2]
    gown[...] = gam
    lane = lax.broadcasted_iota(jnp.int32, (NBF, 128), 1)

    def j_step(n, carry):
        g = lax.rem(n + AGAIN, NGRP)
        slot = lax.rem(n + AGAIN, RING)

        @pl.when((n >= 1) & (n <= AGAIN))
        def _():
            start_group(n - 1, lax.rem(n - 1 + AGAIN, RING))

        @pl.when(n >= RING)
        def _():
            wait_group(g, slot)
        gv = gown[:, 0:NQ]
        acc = jt[...]
        for j in range(GRP):
            x = ring[slot * GRP + j]
            col = jnp.sum(x * gv, axis=1, keepdims=True)
            acc = jnp.where(lane == g * GRP + j, col, acc)
        jt[...] = acc
        k_self(ahead + 2 * n)
        k_self(ahead + 2 * n + 1)
        return carry

    lax.fori_loop(0, NGRP, j_step, 0)

    lane88 = lax.broadcasted_iota(jnp.int32, (RPAD, 128), 1)

    def columns(first, second):
        a = jnp.where(s == 0, first, second)
        b = pltpu.roll(jnp.where(s == 0, second, first), ROWS, 1)
        return jnp.concatenate([jnp.where(lane88 < ROWS, a, b), b], axis=1)[:, 0:HALF]

    jrows = jnp.transpose(jt[...])[0:RPAD]
    j0 = 2.0 * jrows[:, 0:HALF]
    j1 = 2.0 * jrows[:, HALF:2 * HALF]
    kself = columns(ks[:, 0:128], ks[:, 128:256])
    h0 = j0 - jnp.where(p == 0, kself, 0.0)
    h1 = j1 - jnp.where(p == 1, kself, 0.0)
    rsend[:, 0:HALF] = jnp.where(y == 0, h1, h0)
    base = jnp.where(y == 0, h0, h1)
    ks[:, 0:HALF] = base
    r_copy = remote(rsend, rrecv, r_s, r_r, dev(yo, o))
    r_copy.start()

    def early_wait(g, carry):
        early_copy(g).wait_recv()
        return carry

    for g in range(FIRST):
        first_copy(g).wait_recv()
        early_rest(g).wait_recv()
    lax.fori_loop(FIRST, EARLY, early_wait, 0)

    def k_cross(i, moved):
        _, stack = both([t4[keep + k, i] for k in range(2)], [sb[keep + k, i] for k in range(2)])
        return full_nt(jnp.concatenate(moved, axis=1), stack)

    def r_step(c, carry):
        late_copy(c).wait_recv()
        for di in range(ICH):
            i = c * ICH + di
            kr[:, 0:128 + RPAD] += k_cross(i, [rb[k, i, 0:MAIN] for k in range(2)])
        return carry

    lax.fori_loop(0, NCH, r_step, 0)

    def sends(src, lo, n, base):
        rows = pl.ds(lo, n)
        left, right = pl.ds(0, 128), pl.ds(128, 128)
        ss = 3 * (base // 5)
        return (remote(src, pf.at[0, rows], p_s.at[ss], p_r.at[base], dev(y, opp)),
                remote(src, pf.at[1, rows], p_s.at[ss], p_r.at[base + 1], dev(yo, opp)),
                remote(src.at[:, left], ph.at[0, rows], p_s.at[ss + 1], p_r.at[base + 2], dev(yo, o)),
                remote(src.at[:, right], ph.at[1, rows], p_s.at[ss + 2], p_r.at[base + 3], dev(y, sib)),
                remote(src.at[:, right], ph.at[2, rows], p_s.at[ss + 2], p_r.at[base + 4], dev(yo, sib)))

    main = sends(kr, 0, MAIN, 0)
    last = sends(kl, MAIN, GRP, 5)

    @pl.when(y == p)
    def _():
        for k in (0, 4, 2):
            main[k].start()

    @pl.when(y != p)
    def _():
        main[1].start()
        main[3].start()

    def last_step(n, carry):
        for c in range(len(CUTS) - 1):
            @pl.when(n == CUTS[c] // ICH)
            def _():
                last_copy(c).wait_recv()
        gap = jnp.zeros((GRP - TAIL, 128), f32)
        acc = kl[:, 0:128 + RPAD]
        for di in range(ICH):
            i = n * ICH + di
            acc += k_cross(i, [jnp.concatenate([rl[k, pl.ds(TAIL * i, TAIL), :], gap], axis=0) for k in range(2)])
        kl[:, 0:128 + RPAD] = acc
        return carry

    lax.fori_loop(0, NCH, last_step, 0)

    @pl.when(y == p)
    def _():
        for k in (0, 4, 2):
            last[k].start()
        r_copy.wait()
        out[...] = (ks[:, 0:HALF] + rrecv[:, 0:HALF])[0:ROWS]
        for k in (0, 4, 2):
            main[k].wait_send()
            last[k].wait_send()

    @pl.when(y != p)
    def _():
        last[1].start()
        last[3].start()
        r_copy.wait()

        def turn(x):
            return jnp.transpose(jnp.concatenate([x, jnp.zeros((40, 128), f32)], axis=0))[0:RPAD]

        for k in (3, 2, 4):
            main[k].wait_recv()
        for k in (0, 1):
            main[k].wait_recv()
        for k in (3, 2, 4):
            last[k].wait_recv()
        mine_opp = jnp.concatenate([kr[:, 0:128], kl[:, 0:128]], axis=0)
        col_opp = turn(mine_opp + ph[0])
        col_sib = turn(ph[1] + ph[2])
        for k in (0, 1):
            last[k].wait_recv()
        block_a = (pf[0, :, 0:128] + pf[1, :, 0:128]) + col_opp
        block_b = (pf[0, :, 128:256] + pf[1, :, 128:256]) + col_sib
        res = (ks[:, 0:HALF] + rrecv[:, 0:HALF]) - columns(block_a, block_b)
        out[...] = res[0:ROWS]
        for k in (1, 3):
            main[k].wait_send()
            last[k].wait_send()

    def sends_done(g, carry):
        sib_copy(g).wait_send()
        return carry

    lax.fori_loop(0, NGRP, sends_done, 0)

    def early_done(g, carry):
        early_copy(g).wait_send()
        return carry

    for g in range(FIRST):
        first_copy(g).wait_send()
        early_rest(g).wait_send()
    lax.fori_loop(FIRST, EARLY, early_done, 0)

    def late_done(c, carry):
        late_copy(c).wait_send()
        return carry

    lax.fori_loop(0, NCH, late_done, 0)

    for c in range(len(CUTS) - 1):
        last_copy(c).wait_send()


def solution(mesh):
    sem = pltpu.SemaphoreType.DMA

    def local_fock(fit_loc, orbitals):
        bt = jnp.transpose(fit_loc, (1, 2, 0))
        ct = jnp.transpose(orbitals)
        return pl.pallas_call(
            kernel,
            out_shape=pltpu.VMEM((ROWS, HALF), f32),
            in_specs=[pl.BlockSpec(memory_space=pl.ANY), pl.BlockSpec(memory_space=pl.ANY)],
            out_specs=pl.BlockSpec(memory_space=pltpu.VMEM),
            scratch_shapes=[
                pltpu.VMEM((RING * GRP, NBF, NQ), f32),
                pltpu.VMEM((NOCC, NBF), f32),
                pltpu.VMEM((FIRST * GRP, NBF, 128), f32),
                pltpu.VMEM((FIRST * NOCC * GRP, 128), f32),
                pltpu.VMEM((QT, NOCC * RPAD, 128), f32),
                pltpu.VMEM((QT, NOCC, RPAD, 128), f32),
                pltpu.VMEM((2, NOCC, MAIN, 128), f32),
                pltpu.VMEM((QT, DENSE, 128), f32),
                pltpu.VMEM((2, DENSE, 128), f32),
                pltpu.VMEM((32, 512), f32),
                pltpu.VMEM((96, NBF), bf16),
                pltpu.VMEM((32, 128), f32),
                pltpu.VMEM((1, 512), f32),
                pltpu.VMEM((3, 1, 512), f32),
                pltpu.VMEM((NBF, 128), f32),
                pltpu.VMEM((RPAD, 256), f32),
                pltpu.VMEM((MAIN, 256), f32),
                pltpu.VMEM((GRP, 256), f32),
                pltpu.VMEM((RPAD, 256), f32),
                pltpu.VMEM((RPAD, 256), f32),
                pltpu.VMEM((2, RPAD, 256), f32),
                pltpu.VMEM((3, RPAD, 128), f32),
                sem((RING * GRP,)), sem, sem((FIRST,)), sem((FIRST,)), sem((FIRST,)), sem((NGRP,)), sem((NGRP,)), sem((EARLY + NCH,)), sem((EARLY + NCH,)),
                sem((len(CUTS) - 1,)), sem((len(CUTS) - 1,)),
                sem((3,)), sem((3,)), sem, sem, sem((6,)), sem((10,)),
            ],
            compiler_params=pltpu.CompilerParams(collective_id=0, has_side_effects=True,
                                                 vmem_limit_bytes=63 << 20),
            name='fock',
        )(bt, ct)

    spec_fit = P(('sys', 'aux'), 'orb', None)
    spec_orbitals = P('sys', None)
    spec_out = P(('sys', 'orb'), 'aux')
    return jax.shard_map(local_fock, mesh=mesh, in_specs=(spec_fit, spec_orbitals), out_specs=spec_out, check_vma=False)
```

```python
import jax
import jax.numpy as jnp
from jax import lax
from jax.experimental import pallas as pl
from jax.experimental.pallas import tpu as pltpu
from jax.sharding import PartitionSpec as P

f32 = jnp.float32
bf16 = jnp.bfloat16

NOCC = 30
ROWS = 87
RPAD = 88
NBF = 348
NQ = 510
QT = 4
GRP = 8
NGRP = 11
RING = 7
AHEAD = 2
AGAIN = NGRP - RING
EARLY = 6
FIRST = 2
ICH = 3
NCH = NOCC // ICH
LATE = 6
MAIN = RPAD - GRP
TAIL = ROWS - MAIN
DENSE = 216
CUTS = (0, 3, 6, 9, 12, 15, 18, 21, 24, 27, 30)
HALF = 174


def pieces(x):
    hi = x.astype(bf16)
    rest = x - hi.astype(f32)
    mid = rest.astype(bf16)
    low = (rest - mid.astype(f32)).astype(bf16)
    return hi, mid, low


def pieces32(x):
    hi = x.astype(bf16).astype(f32)
    rest = x - hi
    mid = rest.astype(bf16).astype(f32)
    return hi, mid, rest - mid


def dot_nt(a, b):
    return lax.dot_general(a, b, (((1,), (1,)), ((), ())), preferred_element_type=f32)


def full_nt(a, b):
    n = a.shape[0]
    ah, am, al = pieces32(a)
    bh, bm, bl = pieces32(b)
    first = dot_nt(jnp.concatenate([ah, am, al], axis=0), bh)
    second = dot_nt(jnp.concatenate([ah, am], axis=0), bm)
    third = dot_nt(ah, bl)
    small = (first[2 * n:] + second[n:]) + third
    return first[:n] + ((first[n:2 * n] + second[:n]) + small)


def kernel(bt, ct_hbm, out, ring, ct, fb, e0, tb, sb, rb, lt, rl, gacc, cst, cown, gown, grecv, jt, ks, kr, kl, rsend, rrecv,
           pf, ph, dma_sem, ct_sem, fb_sem, d2d_s, d2d_r, ici_s, early_r, late_r, last_r, g_s, g_r, r_s, r_r, p_s, p_r):
    y = lax.axis_index('aux')
    o = lax.axis_index('orb')
    p = o // 2
    s = lax.rem(o, 2)
    sib = o + 1 - 2 * s
    opp = lax.rem(o + 2, 4)
    opp_sib = 3 - o
    yo = 1 - y
    keep = 2 * p
    give = 2 * (1 - p)

    def dev(yy, oo):
        return {'aux': yy, 'orb': oo}

    def remote(src, dst, ssem, rsem, to):
        return pltpu.make_async_remote_copy(src_ref=src, dst_ref=dst, send_sem=ssem, recv_sem=rsem,
                                            device_id=to, device_id_type=pl.DeviceIdType.MESH)

    def load(g, slot):
        return pltpu.make_async_copy(bt.at[pl.ds(g * GRP, GRP)], ring.at[pl.ds(slot * GRP, GRP)], dma_sem.at[slot])

    def tail_load():
        slot = (NGRP - 1) % RING
        return pltpu.make_async_copy(bt.at[pl.ds(MAIN, TAIL)], ring.at[pl.ds(slot * GRP, TAIL)], dma_sem.at[slot])

    def first_load(g):
        lanes = pl.ds(pl.multiple_of(give * 128, 128), 128)
        rows = pl.ds(g * GRP, GRP)
        return pltpu.make_async_copy(bt.at[rows, :, lanes], fb.at[rows], fb_sem)

    ct_copy = pltpu.make_async_copy(ct_hbm, ct, ct_sem)
    ct_copy.start()
    first_load(0).start()
    for g in range(AHEAD):
        load(g, g).start(priority=1)

    barrier = pltpu.get_barrier_semaphore()
    peers = [(y, sib), (y, opp), (y, opp_sib), (yo, o), (yo, sib), (yo, opp), (yo, opp_sib)]
    for peer in peers:
        pl.semaphore_signal(barrier, inc=1, device_id=dev(*peer), device_id_type=pl.DeviceIdType.MESH)

    t4 = tb.reshape(QT, NOCC, RPAD, 128)

    def cross(src, dst, rsem):
        return remote(src, dst, ici_s.at[0], rsem, dev(y, opp))

    def early_copy(g):
        rows = pl.ds(pl.multiple_of(g * GRP, GRP), GRP)
        return cross(t4.at[pl.ds(give, 2), :, rows], rb.at[:, :, rows], early_r)

    def early_rest(g):
        rows = pl.ds(pl.multiple_of(g * GRP, GRP), GRP)
        return cross(t4.at[pl.ds(give + 1, 1), :, rows], rb.at[pl.ds(1, 1), :, rows], early_r)

    e4 = e0.reshape(FIRST, NOCC, GRP, 128)

    def first_copy(g):
        return cross(e4.at[g], rb.at[0, :, pl.ds(g * GRP, GRP)], early_r)

    def late_copy(c):
        orbs = pl.ds(c * LATE, LATE)
        rows = pl.ds(EARLY * GRP, MAIN - EARLY * GRP)
        return cross(t4.at[pl.ds(give, 2), orbs, rows], rb.at[:, orbs, rows], late_r.at[c])

    def last_copy(c):
        lo, hi = (-(-TAIL * CUTS[k] // GRP) * GRP for k in (c, c + 1))
        rows = pl.ds(lo, hi - lo)
        return remote(lt.at[pl.ds(give, 2), rows], rl.at[:, rows], ici_s.at[1], last_r.at[c], dev(y, opp))

    early_rows = pl.ds(0, EARLY * GRP)
    early_all = cross(t4.at[pl.ds(give, 2), :, early_rows], rb.at[:, :, early_rows], early_r)
    main_all = cross(t4.at[pl.ds(give, 2), :, pl.ds(0, MAIN)], rb, early_r)
    last_all = remote(lt.at[pl.ds(give, 2)], rl, ici_s.at[1], last_r.at[0], dev(y, opp))
    sib_all = remote(t4, sb, d2d_s, d2d_r, dev(y, sib))
    g_all = remote(grecv, grecv, g_s, g_r, dev(y, sib))

    def sib_copy(g):
        rows = pl.ds(pl.multiple_of(g * GRP, GRP), GRP)
        return remote(t4.at[:, :, rows], sb.at[:, :, rows], d2d_s, d2d_r, dev(y, sib))

    ct_copy.wait()
    c = jnp.concatenate([ct[...], jnp.zeros((2, NBF), f32)], axis=0)
    cst[...] = jnp.concatenate(pieces(c), axis=0)
    def t_rows(x):
        r = None
        for piece in pieces(x):
            term = jnp.dot(cst[...], piece, preferred_element_type=f32)
            r = term if r is None else r + term
        return r[0:32] + r[32:64] + r[64:96]

    for g in range(FIRST):
        first_load(g).wait()
        if g + 1 < FIRST:
            first_load(g + 1).start()
        for j in range(GRP):
            e0[pl.ds(g * NOCC * GRP + j, NOCC, stride=GRP), :] = t_rows(fb[g * GRP + j])[:NOCC]
        if g == 0:
            pl.semaphore_wait(barrier, len(peers))
        first_copy(g).start()

    mine = c[:, 0:ROWS]
    for b in range(1, 4):
        mine = jnp.where(o == b, c[:, b * ROWS:(b + 1) * ROWS], mine)
    cown[...] = jnp.concatenate([mine, jnp.zeros((32, 128 - ROWS), f32)], axis=1)
    gacc[...] = jnp.zeros_like(gacc)
    jt[...] = jnp.zeros_like(jt)
    ks[...] = jnp.zeros_like(ks)
    kr[...] = jnp.zeros_like(kr)
    kl[...] = jnp.zeros_like(kl)

    def t_group(g, rows, dense):
        slot = lax.rem(g, RING)
        if dense:
            tail_load().wait()
        else:
            @pl.when(g + AHEAD < NGRP - 1)
            def _():
                load(g + AHEAD, lax.rem(g + AHEAD, RING)).start(priority=1)

            @pl.when(g + AHEAD == NGRP - 1)
            def _():
                tail_load().start(priority=1)
            load(g, slot).wait()
        cg = pltpu.roll(cown[...], lax.rem(128 - g * GRP, 128), 1)
        for j in range(rows):
            m = g * GRP + j
            t = t_rows(ring[slot * GRP + j])
            gacc[:, 0:NQ] += t * cg[:, j:j + 1]
            for k in range(QT):
                hi = min(NQ, 128 * (k + 1))
                tt = t[:NOCC, 128 * k:hi]
                if hi < 128 * (k + 1):
                    tt = jnp.concatenate([tt, jnp.zeros((NOCC, 128 * (k + 1) - hi), f32)], axis=1)
                tb[k, pl.ds(m, NOCC, stride=RPAD), :] = tt
                if dense:
                    lt[k, pl.ds(j, NOCC, stride=TAIL), :] = tt
        sib_copy(g).start()

    def t_step(g, carry):
        t_group(g, GRP, False)

        @pl.when(g < FIRST)
        def _():
            early_rest(g).start()

        @pl.when((g >= FIRST) & (g < EARLY))
        def _():
            early_copy(g).start()
        return carry

    lax.fori_loop(0, NGRP - 1, t_step, 0)
    for k in range(QT):
        tb[k, pl.ds(ROWS, NOCC, stride=RPAD), :] = jnp.zeros((NOCC, 128), f32)
        lt[k, DENSE - GRP:, :] = jnp.zeros((GRP, 128), f32)
    t_group(NGRP - 1, TAIL, True)

    gown[...] = jnp.sum(gacc[...], axis=0, keepdims=True)
    g_copies = [remote(gown, grecv.at[k], g_s, g_r, dev(y, to))
                for k, to in enumerate((sib, opp, opp_sib))]
    for copy in g_copies:
        copy.start()

    def late_start(c, carry):
        late_copy(c).start()
        return carry

    lax.fori_loop(0, NOCC // LATE, late_start, 0)

    for c in range(len(CUTS) - 1):
        last_copy(c).start()

    sib_all.wait_recv()

    def both(tiles_own, tiles_sib):
        own = jnp.concatenate(tiles_own, axis=1)
        other = jnp.concatenate(tiles_sib, axis=1)
        gap = jnp.zeros((128 - RPAD, own.shape[1]), f32)
        return own, jnp.concatenate([own, gap, other], axis=0)

    def k_self(i):
        own, stack = both([t4[k, i] for k in range(QT)], [sb[k, i] for k in range(QT)])
        res = full_nt(own, stack)
        ks[:, 0:128 + RPAD] += res

    def self_step(i, carry):
        k_self(i)
        return carry

    ahead = NOCC - 2 * NGRP
    lax.fori_loop(0, ahead, self_step, 0)

    g_all.wait()
    gam = gown[...] + grecv[0] + grecv[1] + grecv[2]
    gown[...] = gam
    lane = lax.broadcasted_iota(jnp.int32, (NBF, 128), 1)

    def j_step(n, carry):
        g = lax.rem(n + AGAIN, NGRP)
        slot = lax.rem(n + AGAIN, RING)

        @pl.when((n >= 1) & (n <= AGAIN))
        def _():
            load(n - 1, lax.rem(n - 1 + AGAIN, RING)).start(priority=1)

        @pl.when(n >= RING)
        def _():
            load(g, slot).wait()
        gv = gown[:, 0:NQ]
        acc = jt[...]
        for j in range(GRP):
            x = ring[slot * GRP + j]
            col = jnp.sum(x * gv, axis=1, keepdims=True)
            acc = jnp.where(lane == g * GRP + j, col, acc)
        jt[...] = acc
        k_self(ahead + 2 * n)
        k_self(ahead + 2 * n + 1)
        return carry

    lax.fori_loop(0, NGRP, j_step, 0)

    lane88 = lax.broadcasted_iota(jnp.int32, (RPAD, 128), 1)

    def columns(first, second):
        a = jnp.where(s == 0, first, second)
        b = pltpu.roll(jnp.where(s == 0, second, first), ROWS, 1)
        return jnp.concatenate([jnp.where(lane88 < ROWS, a, b), b], axis=1)[:, 0:HALF]

    jrows = jnp.transpose(jt[...])[0:RPAD]
    j0 = 2.0 * jrows[:, 0:HALF]
    j1 = 2.0 * jrows[:, HALF:2 * HALF]
    kself = columns(ks[:, 0:128], ks[:, 128:256])
    h0 = j0 - jnp.where(p == 0, kself, 0.0)
    h1 = j1 - jnp.where(p == 1, kself, 0.0)
    rsend[:, 0:HALF] = jnp.where(y == 0, h1, h0)
    base = jnp.where(y == 0, h0, h1)
    ks[:, 0:HALF] = base
    r_copy = remote(rsend, rrecv, r_s, r_r, dev(yo, o))
    r_copy.start()

    early_all.wait_recv()

    def k_cross(i, moved):
        _, stack = both([t4[keep + k, i] for k in range(2)], [sb[keep + k, i] for k in range(2)])
        return full_nt(jnp.concatenate(moved, axis=1), stack)

    def r_step(c, carry):
        @pl.when(lax.rem(c, LATE // ICH) == 0)
        def _():
            late_copy(c // (LATE // ICH)).wait_recv()
        for di in range(ICH):
            i = c * ICH + di
            kr[:, 0:128 + RPAD] += k_cross(i, [rb[k, i, 0:MAIN] for k in range(2)])
        return carry

    lax.fori_loop(0, NCH, r_step, 0)

    def sends(src, lo, n, base):
        rows = pl.ds(lo, n)
        left, right = pl.ds(0, 128), pl.ds(128, 128)
        full_s, half_s = p_s.at[base], p_s.at[base + 1]
        full_r, half_r = p_r.at[base], p_r.at[base + 1]
        return (remote(src, pf.at[0, rows], full_s, full_r, dev(y, opp)),
                remote(src, pf.at[1, rows], full_s, full_r, dev(yo, opp)),
                remote(src.at[:, left], ph.at[0, rows], half_s, half_r, dev(yo, o)),
                remote(src.at[:, right], ph.at[1, rows], half_s, half_r, dev(y, sib)),
                remote(src.at[:, right], ph.at[2, rows], half_s, half_r, dev(yo, sib)),
                remote(pf.at[:, rows], pf.at[:, rows], full_s, full_r, dev(y, opp)),
                remote(ph.at[:, rows], ph.at[:, rows], half_s, half_r, dev(y, sib)),
                remote(ph.at[pl.ds(0, 2), rows], ph.at[pl.ds(0, 2), rows], half_s, half_r, dev(y, sib)))

    main = sends(kr, 0, MAIN, 0)
    last = sends(kl, MAIN, GRP, 2)

    @pl.when(y == p)
    def _():
        for k in (0, 4, 2):
            main[k].start()

    @pl.when(y != p)
    def _():
        main[1].start()
        main[3].start()

    sib_all.wait_send()
    main_all.wait_send()

    def last_step(n, carry):
        for c in range(len(CUTS) - 1):
            @pl.when(n == CUTS[c] // ICH)
            def _():
                last_copy(c).wait_recv()
        gap = jnp.zeros((GRP - TAIL, 128), f32)
        acc = kl[:, 0:128 + RPAD]
        for di in range(ICH):
            i = n * ICH + di
            acc += k_cross(i, [jnp.concatenate([rl[k, pl.ds(TAIL * i, TAIL), :], gap], axis=0) for k in range(2)])
        kl[:, 0:128 + RPAD] = acc
        return carry

    lax.fori_loop(0, NCH, last_step, 0)

    def sent():
        last_all.wait_send()

    @pl.when(y == p)
    def _():
        for k in (0, 4, 2):
            last[k].start()
        sent()
        r_copy.wait()
        out[...] = (ks[:, 0:HALF] + rrecv[:, 0:HALF])[0:ROWS]
        for group in (main, last):
            group[0].wait_send()
            group[7].wait_send()

    @pl.when(y != p)
    def _():
        last[1].start()
        last[3].start()
        sent()
        r_copy.wait()

        def turn(x):
            return jnp.transpose(jnp.concatenate([x, jnp.zeros((40, 128), f32)], axis=0))[0:RPAD]

        main[6].wait_recv()
        main[5].wait_recv()
        last[6].wait_recv()
        mine_opp = jnp.concatenate([kr[:, 0:128], kl[:, 0:128]], axis=0)
        col_opp = turn(mine_opp + ph[0])
        col_sib = turn(ph[1] + ph[2])
        last[5].wait_recv()
        block_a = (pf[0, :, 0:128] + pf[1, :, 0:128]) + col_opp
        block_b = (pf[0, :, 128:256] + pf[1, :, 128:256]) + col_sib
        res = (ks[:, 0:HALF] + rrecv[:, 0:HALF]) - columns(block_a, block_b)
        out[...] = res[0:ROWS]
        for group in (main, last):
            group[1].wait_send()
            group[3].wait_send()


def solution(mesh):
    sem = pltpu.SemaphoreType.DMA

    def local_fock(fit_loc, orbitals):
        bt = jnp.transpose(fit_loc, (1, 2, 0))
        ct = jnp.transpose(orbitals)
        return pl.pallas_call(
            kernel,
            out_shape=pltpu.VMEM((ROWS, HALF), f32),
            in_specs=[pl.BlockSpec(memory_space=pl.ANY), pl.BlockSpec(memory_space=pl.ANY)],
            out_specs=pl.BlockSpec(memory_space=pltpu.VMEM),
            scratch_shapes=[
                pltpu.VMEM((RING * GRP, NBF, NQ), f32),
                pltpu.VMEM((NOCC, NBF), f32),
                pltpu.VMEM((FIRST * GRP, NBF, 128), f32),
                pltpu.VMEM((FIRST * NOCC * GRP, 128), f32),
                pltpu.VMEM((QT, NOCC * RPAD, 128), f32),
                pltpu.VMEM((QT, NOCC, RPAD, 128), f32),
                pltpu.VMEM((2, NOCC, MAIN, 128), f32),
                pltpu.VMEM((QT, DENSE, 128), f32),
                pltpu.VMEM((2, DENSE, 128), f32),
                pltpu.VMEM((32, 512), f32),
                pltpu.VMEM((96, NBF), bf16),
                pltpu.VMEM((32, 128), f32),
                pltpu.VMEM((1, 512), f32),
                pltpu.VMEM((3, 1, 512), f32),
                pltpu.VMEM((NBF, 128), f32),
                pltpu.VMEM((RPAD, 256), f32),
                pltpu.VMEM((MAIN, 256), f32),
                pltpu.VMEM((GRP, 256), f32),
                pltpu.VMEM((RPAD, 256), f32),
                pltpu.VMEM((RPAD, 256), f32),
                pltpu.VMEM((2, RPAD, 256), f32),
                pltpu.VMEM((3, RPAD, 128), f32),
                sem((RING,)), sem, sem, sem, sem, sem((2,)), sem, sem((NOCC // LATE,)), sem((len(CUTS) - 1,)),
                sem, sem, sem, sem, sem((4,)), sem((4,)),
            ],
            compiler_params=pltpu.CompilerParams(collective_id=0, has_side_effects=True,
                                                 vmem_limit_bytes=63 << 20),
            name='fock',
        )(bt, ct)

    spec_fit = P(('sys', 'aux'), 'orb', None)
    spec_orbitals = P('sys', None)
    spec_out = P(('sys', 'orb'), 'aux')
    return jax.shard_map(local_fock, mesh=mesh, in_specs=(spec_fit, spec_orbitals), out_specs=spec_out, check_vma=False)
```

```python
import jax
import jax.numpy as jnp
from jax import lax
from jax.experimental import pallas as pl
from jax.experimental.pallas import tpu as pltpu
from jax.sharding import PartitionSpec as P

f32 = jnp.float32
bf16 = jnp.bfloat16

NOCC = 30
ROWS = 87
RPAD = 88
NBF = 348
NQ = 510
QT = 4
GRP = 8
NGRP = 11
RING = 7
AHEAD = 2
AGAIN = NGRP - RING
EARLY = 6
FIRST = 2
ICH = 3
NCH = NOCC // ICH
LATE = 6
MAIN = RPAD - GRP
TAIL = ROWS - MAIN
DENSE = 216
LSTEP = 2
CUTS = [-(-TAIL * i // GRP) * GRP for i in range(0, NOCC + 1, LSTEP)]
SIZES = [b - a for a, b in zip(CUTS, CUTS[1:])]
HALF = 174


def pieces(x):
    hi = x.astype(bf16)
    rest = x - hi.astype(f32)
    mid = rest.astype(bf16)
    low = (rest - mid.astype(f32)).astype(bf16)
    return hi, mid, low


def pieces32(x):
    hi = x.astype(bf16).astype(f32)
    rest = x - hi
    mid = rest.astype(bf16).astype(f32)
    return hi, mid, rest - mid


def dot_nt(a, b):
    return lax.dot_general(a, b, (((1,), (1,)), ((), ())), preferred_element_type=f32)


def full_nt(a, b):
    n = a.shape[0]
    ah, am, al = pieces32(a)
    bh, bm, bl = pieces32(b)
    first = dot_nt(jnp.concatenate([ah, am, al], axis=0), bh)
    second = dot_nt(jnp.concatenate([ah, am], axis=0), bm)
    third = dot_nt(ah, bl)
    small = (first[2 * n:] + second[n:]) + third
    return first[:n] + ((first[n:2 * n] + second[:n]) + small)


def kernel(bt, ct_hbm, out, ring, ct, fb, e0, tb, sb, rb, lt, rl, gacc, cst, cown, gown, grecv, jt, ks, kr, kl, rsend, rrecv,
           pf, ph, dma_sem, ct_sem, fb_sem, d2d_s, d2d_r, ici_s, early_r, late_r, last_r, g_s, g_r, r_s, r_r, p_s, p_r):
    y = lax.axis_index('aux')
    o = lax.axis_index('orb')
    p = o // 2
    s = lax.rem(o, 2)
    sib = o + 1 - 2 * s
    opp = lax.rem(o + 2, 4)
    opp_sib = 3 - o
    yo = 1 - y
    keep = 2 * p
    give = 2 * (1 - p)

    def dev(yy, oo):
        return {'aux': yy, 'orb': oo}

    def remote(src, dst, ssem, rsem, to):
        return pltpu.make_async_remote_copy(src_ref=src, dst_ref=dst, send_sem=ssem, recv_sem=rsem,
                                            device_id=to, device_id_type=pl.DeviceIdType.MESH)

    def load(g, slot):
        return pltpu.make_async_copy(bt.at[pl.ds(g * GRP, GRP)], ring.at[pl.ds(slot * GRP, GRP)], dma_sem.at[lax.rem(g, 4)])

    def tail_load():
        slot = (NGRP - 1) % RING
        return pltpu.make_async_copy(bt.at[pl.ds(MAIN, TAIL)], ring.at[pl.ds(slot * GRP, TAIL)], dma_sem.at[(NGRP - 1) % 4])

    def first_load(g, h):
        lanes = pl.ds(pl.multiple_of(give * 128, 128), 128)
        rows = pl.ds(g * GRP + h * (GRP // 2), GRP // 2)
        return pltpu.make_async_copy(bt.at[rows, :, lanes], fb.at[rows], fb_sem.at[h])

    ct_copy = pltpu.make_async_copy(ct_hbm, ct, ct_sem)
    ct_copy.start()
    first_load(0, 0).start()
    first_load(0, 1).start()
    for g in range(AHEAD):
        load(g, g).start(priority=1)

    barrier = pltpu.get_barrier_semaphore()
    peers = [(y, sib), (y, opp), (y, opp_sib), (yo, o), (yo, sib), (yo, opp), (yo, opp_sib)]
    for peer in peers:
        pl.semaphore_signal(barrier, inc=1, device_id=dev(*peer), device_id_type=pl.DeviceIdType.MESH)

    t4 = tb.reshape(QT, NOCC, RPAD, 128)

    def cross(src, dst, rsem):
        return remote(src, dst, ici_s.at[0], rsem, dev(y, opp))

    def early_copy(g):
        rows = pl.ds(pl.multiple_of(g * GRP, GRP), GRP)
        return cross(t4.at[pl.ds(give, 2), :, rows], rb.at[:, :, rows], early_r)

    def early_rest(g):
        rows = pl.ds(pl.multiple_of(g * GRP, GRP), GRP)
        return cross(t4.at[pl.ds(give + 1, 1), :, rows], rb.at[pl.ds(1, 1), :, rows], early_r)

    e4 = e0.reshape(FIRST, NOCC, GRP, 128)

    def first_copy(g):
        return cross(e4.at[g], rb.at[0, :, pl.ds(g * GRP, GRP)], early_r)

    def late_copy(c):
        orbs = pl.ds(c * LATE, LATE)
        rows = pl.ds(EARLY * GRP, MAIN - EARLY * GRP)
        return cross(t4.at[pl.ds(give, 2), orbs, rows], rb.at[:, orbs, rows], late_r.at[c])

    def last_copy(c):
        rows = pl.ds(CUTS[c], SIZES[c])
        return remote(lt.at[pl.ds(give, 2), rows], rl.at[:, rows], ici_s.at[1], last_r.at[c], dev(y, opp))

    early_rows = pl.ds(0, EARLY * GRP)
    early_all = cross(t4.at[pl.ds(give, 2), :, early_rows], rb.at[:, :, early_rows], early_r)
    main_all = cross(t4.at[pl.ds(give, 2), :, pl.ds(0, MAIN)], rb, early_r)
    last_all = remote(lt.at[pl.ds(give, 2)], rl, ici_s.at[1], last_r.at[0], dev(y, opp))
    sib_all = remote(t4, sb, d2d_s, d2d_r, dev(y, sib))
    g_all = remote(grecv, grecv, g_s, g_r, dev(y, sib))

    def sib_copy(g):
        rows = pl.ds(pl.multiple_of(g * GRP, GRP), GRP)
        return remote(t4.at[:, :, rows], sb.at[:, :, rows], d2d_s, d2d_r, dev(y, sib))

    ct_copy.wait()
    c = jnp.concatenate([ct[...], jnp.zeros((2, NBF), f32)], axis=0)
    cst[...] = jnp.concatenate(pieces(c), axis=0)
    def t_rows(x):
        r = None
        for piece in pieces(x):
            term = jnp.dot(cst[...], piece, preferred_element_type=f32)
            r = term if r is None else r + term
        return r[0:32] + r[32:64] + r[64:96]

    for g in range(FIRST):
        for h in range(2):
            first_load(g, h).wait()
            if g + 1 < FIRST and h == 1:
                first_load(g + 1, 0).start()
                first_load(g + 1, 1).start()
            for j in range(h * GRP // 2, (h + 1) * GRP // 2):
                e0[pl.ds(g * NOCC * GRP + j, NOCC, stride=GRP), :] = t_rows(fb[g * GRP + j])[:NOCC]
        if g == 0:
            pl.semaphore_wait(barrier, len(peers))
        first_copy(g).start()

    mine = c[:, 0:ROWS]
    for b in range(1, 4):
        mine = jnp.where(o == b, c[:, b * ROWS:(b + 1) * ROWS], mine)
    cown[...] = jnp.concatenate([mine, jnp.zeros((32, 128 - ROWS), f32)], axis=1)
    gacc[...] = jnp.zeros_like(gacc)
    jt[...] = jnp.zeros_like(jt)
    ks[...] = jnp.zeros_like(ks)
    kr[...] = jnp.zeros_like(kr)
    kl[...] = jnp.zeros_like(kl)

    def t_group(g, rows, dense):
        slot = lax.rem(g, RING)
        if dense:
            tail_load().wait()
        else:
            @pl.when(g + AHEAD < NGRP - 1)
            def _():
                load(g + AHEAD, lax.rem(g + AHEAD, RING)).start(priority=1)

            @pl.when(g + AHEAD == NGRP - 1)
            def _():
                tail_load().start(priority=1)
            load(g, slot).wait()
        cg = pltpu.roll(cown[...], lax.rem(128 - g * GRP, 128), 1)
        for j in range(rows):
            m = g * GRP + j
            t = t_rows(ring[slot * GRP + j])
            gacc[:, 0:NQ] += t * cg[:, j:j + 1]
            for k in range(QT):
                hi = min(NQ, 128 * (k + 1))
                tt = t[:NOCC, 128 * k:hi]
                if hi < 128 * (k + 1):
                    tt = jnp.concatenate([tt, jnp.zeros((NOCC, 128 * (k + 1) - hi), f32)], axis=1)
                tb[k, pl.ds(m, NOCC, stride=RPAD), :] = tt
                if dense:
                    lt[k, pl.ds(j, NOCC, stride=TAIL), :] = tt
        sib_copy(g).start()

    def t_step(g, carry):
        t_group(g, GRP, False)

        @pl.when(g < FIRST)
        def _():
            early_rest(g).start()

        @pl.when((g >= FIRST) & (g < EARLY))
        def _():
            early_copy(g).start()
        return carry

    lax.fori_loop(0, NGRP - 1, t_step, 0)
    for k in range(QT):
        tb[k, pl.ds(ROWS, NOCC, stride=RPAD), :] = jnp.zeros((NOCC, 128), f32)
        lt[k, DENSE - GRP:, :] = jnp.zeros((GRP, 128), f32)
    t_group(NGRP - 1, TAIL, True)

    gown[...] = jnp.sum(gacc[...], axis=0, keepdims=True)
    g_copies = [remote(gown, grecv.at[k], g_s, g_r, dev(y, to))
                for k, to in enumerate((sib, opp, opp_sib))]
    for copy in g_copies:
        copy.start()

    def late_start(c, carry):
        late_copy(c).start()
        return carry

    lax.fori_loop(0, NOCC // LATE, late_start, 0)

    for c in range(len(CUTS) - 1):
        last_copy(c).start()

    sib_all.wait_recv()

    def both(tiles_own, tiles_sib):
        own = jnp.concatenate(tiles_own, axis=1)
        other = jnp.concatenate(tiles_sib, axis=1)
        gap = jnp.zeros((128 - RPAD, own.shape[1]), f32)
        return own, jnp.concatenate([own, gap, other], axis=0)

    def k_self(i):
        own, stack = both([t4[k, i] for k in range(QT)], [sb[k, i] for k in range(QT)])
        res = full_nt(own, stack)
        ks[:, 0:128 + RPAD] += res

    def self_step(i, carry):
        k_self(i)
        return carry

    ahead = NOCC - 2 * NGRP
    lax.fori_loop(0, ahead, self_step, 0)

    g_all.wait()
    gam = gown[...] + grecv[0] + grecv[1] + grecv[2]
    gown[...] = gam
    lane = lax.broadcasted_iota(jnp.int32, (NBF, 128), 1)

    def j_step(n, carry):
        g = lax.rem(n + AGAIN, NGRP)
        slot = lax.rem(n + AGAIN, RING)

        @pl.when((n >= 1) & (n <= AGAIN))
        def _():
            load(n - 1, lax.rem(n - 1 + AGAIN, RING)).start(priority=1)

        @pl.when(n >= RING)
        def _():
            load(g, slot).wait()
        gv = gown[:, 0:NQ]
        acc = jt[...]
        for j in range(GRP):
            x = ring[slot * GRP + j]
            col = jnp.sum(x * gv, axis=1, keepdims=True)
            acc = jnp.where(lane == g * GRP + j, col, acc)
        jt[...] = acc
        k_self(ahead + 2 * n)
        k_self(ahead + 2 * n + 1)
        return carry

    lax.fori_loop(0, NGRP, j_step, 0)

    lane88 = lax.broadcasted_iota(jnp.int32, (RPAD, 128), 1)

    def columns(first, second):
        a = jnp.where(s == 0, first, second)
        b = pltpu.roll(jnp.where(s == 0, second, first), ROWS, 1)
        return jnp.concatenate([jnp.where(lane88 < ROWS, a, b), b], axis=1)[:, 0:HALF]

    jrows = jnp.transpose(jt[...])[0:RPAD]
    j0 = 2.0 * jrows[:, 0:HALF]
    j1 = 2.0 * jrows[:, HALF:2 * HALF]
    kself = columns(ks[:, 0:128], ks[:, 128:256])
    h0 = j0 - jnp.where(p == 0, kself, 0.0)
    h1 = j1 - jnp.where(p == 1, kself, 0.0)
    rsend[:, 0:HALF] = jnp.where(y == 0, h1, h0)
    base = jnp.where(y == 0, h0, h1)
    ks[:, 0:HALF] = base
    r_copy = remote(rsend, rrecv, r_s, r_r, dev(yo, o))
    r_copy.start()

    early_all.wait_recv()

    def k_cross(i, moved):
        _, stack = both([t4[keep + k, i] for k in range(2)], [sb[keep + k, i] for k in range(2)])
        return full_nt(jnp.concatenate(moved, axis=1), stack)

    def r_step(c, carry):
        @pl.when(lax.rem(c, LATE // ICH) == 0)
        def _():
            late_copy(c // (LATE // ICH)).wait_recv()
        for di in range(ICH):
            i = c * ICH + di
            kr[:, 0:128 + RPAD] += k_cross(i, [rb[k, i, 0:MAIN] for k in range(2)])
        return carry

    lax.fori_loop(0, NCH, r_step, 0)

    def sends(src, lo, n, base):
        rows = pl.ds(lo, n)
        left, right = pl.ds(0, 128), pl.ds(128, 128)
        full_s, half_s = p_s.at[0], p_s.at[1]
        full_r, half_r = p_r.at[base], p_r.at[base + 1]
        return (remote(src, pf.at[0, rows], full_s, full_r, dev(y, opp)),
                remote(src, pf.at[1, rows], full_s, full_r, dev(yo, opp)),
                remote(src.at[:, left], ph.at[0, rows], half_s, half_r, dev(yo, o)),
                remote(src.at[:, right], ph.at[1, rows], half_s, half_r, dev(y, sib)),
                remote(src.at[:, right], ph.at[2, rows], half_s, half_r, dev(yo, sib)),
                remote(pf.at[:, rows], pf.at[:, rows], full_s, full_r, dev(y, opp)),
                remote(ph.at[:, rows], ph.at[:, rows], half_s, half_r, dev(y, sib)),
                remote(ph.at[pl.ds(0, 2), rows], ph.at[pl.ds(0, 2), rows], half_s, half_r, dev(y, sib)))

    main = sends(kr, 0, MAIN, 0)
    last = sends(kl, MAIN, GRP, 2)
    whole = sends(rsend, 0, RPAD, 0)

    @pl.when(y == p)
    def _():
        for k in (0, 4, 2):
            main[k].start()

    @pl.when(y != p)
    def _():
        main[1].start()
        main[3].start()

    sib_all.wait_send()
    main_all.wait_send()

    def last_step(n, carry):
        for size in sorted(set(SIZES)):
            hit = n < 0
            for c, rows in enumerate(SIZES):
                if rows == size:
                    hit = hit | (n == c)

            @pl.when(hit)
            def _():
                part = pl.ds(0, size)
                remote(lt.at[pl.ds(give, 2), part], rl.at[:, part], ici_s.at[1], last_r.at[n], dev(y, opp)).wait_recv()
        gap = jnp.zeros((GRP - TAIL, 128), f32)
        own, other, moved = [], [], []
        for di in range(LSTEP):
            i = n * LSTEP + di
            for k in range(2):
                own.append(t4[keep + k, i])
                other.append(sb[keep + k, i])
                moved.append(jnp.concatenate([rl[k, pl.ds(TAIL * i, TAIL), :], gap], axis=0))
        moved = jnp.concatenate(moved, axis=1)
        kl[:, 0:RPAD] += full_nt(moved, jnp.concatenate(own, axis=1))
        kl[:, 128:128 + RPAD] += full_nt(moved, jnp.concatenate(other, axis=1))
        return carry

    lax.fori_loop(0, NOCC // LSTEP, last_step, 0)

    def sent():
        last_all.wait_send()

    @pl.when(y == p)
    def _():
        for k in (0, 4, 2):
            last[k].start()
        sent()
        r_copy.wait()
        out[...] = (ks[:, 0:HALF] + rrecv[:, 0:HALF])[0:ROWS]
        whole[0].wait_send()
        whole[7].wait_send()

    @pl.when(y != p)
    def _():
        last[1].start()
        last[3].start()
        sent()
        r_copy.wait()

        def turn(x):
            return jnp.transpose(jnp.concatenate([x, jnp.zeros((40, 128), f32)], axis=0))[0:RPAD]

        main[6].wait_recv()
        main[5].wait_recv()
        last[6].wait_recv()
        mine_opp = jnp.concatenate([kr[:, 0:128], kl[:, 0:128]], axis=0)
        col_opp = turn(mine_opp + ph[0])
        col_sib = turn(ph[1] + ph[2])
        last[5].wait_recv()
        block_a = (pf[0, :, 0:128] + pf[1, :, 0:128]) + col_opp
        block_b = (pf[0, :, 128:256] + pf[1, :, 128:256]) + col_sib
        res = (ks[:, 0:HALF] + rrecv[:, 0:HALF]) - columns(block_a, block_b)
        out[...] = res[0:ROWS]
        whole[0].wait_send()
        whole[3].wait_send()


def solution(mesh):
    sem = pltpu.SemaphoreType.DMA

    def local_fock(fit_loc, orbitals):
        bt = jnp.transpose(fit_loc, (1, 2, 0))
        ct = jnp.transpose(orbitals)
        return pl.pallas_call(
            kernel,
            out_shape=pltpu.VMEM((ROWS, HALF), f32),
            in_specs=[pl.BlockSpec(memory_space=pl.ANY), pl.BlockSpec(memory_space=pl.ANY)],
            out_specs=pl.BlockSpec(memory_space=pltpu.VMEM),
            scratch_shapes=[
                pltpu.VMEM((RING * GRP, NBF, NQ), f32),
                pltpu.VMEM((NOCC, NBF), f32),
                pltpu.VMEM((FIRST * GRP, NBF, 128), f32),
                pltpu.VMEM((FIRST * NOCC * GRP, 128), f32),
                pltpu.VMEM((QT, NOCC * RPAD, 128), f32),
                pltpu.VMEM((QT, NOCC, RPAD, 128), f32),
                pltpu.VMEM((2, NOCC, MAIN, 128), f32),
                pltpu.VMEM((QT, DENSE, 128), f32),
                pltpu.VMEM((2, DENSE, 128), f32),
                pltpu.VMEM((32, 512), f32),
                pltpu.VMEM((96, NBF), bf16),
                pltpu.VMEM((32, 128), f32),
                pltpu.VMEM((1, 512), f32),
                pltpu.VMEM((3, 1, 512), f32),
                pltpu.VMEM((NBF, 128), f32),
                pltpu.VMEM((RPAD, 256), f32),
                pltpu.VMEM((MAIN, 256), f32),
                pltpu.VMEM((GRP, 256), f32),
                pltpu.VMEM((RPAD, 256), f32),
                pltpu.VMEM((RPAD, 256), f32),
                pltpu.VMEM((2, RPAD, 256), f32),
                pltpu.VMEM((3, RPAD, 128), f32),
                sem((4,)), sem, sem((2,)), sem, sem, sem((2,)), sem, sem((NOCC // LATE,)), sem((len(CUTS) - 1,)),
                sem, sem, sem, sem, sem((2,)), sem((4,)),
            ],
            compiler_params=pltpu.CompilerParams(collective_id=0, has_side_effects=True,
                                                 vmem_limit_bytes=63 << 20),
            name='fock',
        )(bt, ct)

    spec_fit = P(('sys', 'aux'), 'orb', None)
    spec_orbitals = P('sys', None)
    spec_out = P(('sys', 'orb'), 'aux')
    return jax.shard_map(local_fock, mesh=mesh, in_specs=(spec_fit, spec_orbitals), out_specs=spec_out, check_vma=False)
```

```python
import jax
import jax.numpy as jnp
from jax import lax
from jax.experimental import pallas as pl
from jax.experimental.pallas import tpu as pltpu
from jax.sharding import PartitionSpec as P

f32 = jnp.float32
bf16 = jnp.bfloat16

NOCC = 30
ROWS = 87
RPAD = 88
NBF = 348
NQ = 510
QT = 4
GRP = 8
NGRP = 11
RING = 7
AHEAD = 2
AGAIN = NGRP - RING
EARLY = 6
FIRST = 2
ICH = 3
NCH = NOCC // ICH
LATE = 6
MAIN = RPAD - GRP
TAIL = ROWS - MAIN
DENSE = 216
LSTEP = 2
SENDS = (0, 4, 8, 12, 16, 18, 20, 22, 24, 26, 28, NOCC)
CUTS = [-(-TAIL * i // GRP) * GRP for i in SENDS]
SIZES = [b - a for a, b in zip(CUTS, CUTS[1:])]
HALF = 174


def pieces(x):
    hi = x.astype(bf16)
    rest = x - hi.astype(f32)
    mid = rest.astype(bf16)
    low = (rest - mid.astype(f32)).astype(bf16)
    return hi, mid, low


def pieces32(x):
    hi = x.astype(bf16).astype(f32)
    rest = x - hi
    mid = rest.astype(bf16).astype(f32)
    return hi, mid, rest - mid


def dot_nt(a, b):
    return lax.dot_general(a, b, (((1,), (1,)), ((), ())), preferred_element_type=f32)


def full_nt(a, b):
    n = a.shape[0]
    ah, am, al = pieces32(a)
    bh, bm, bl = pieces32(b)
    first = dot_nt(jnp.concatenate([ah, am, al], axis=0), bh)
    second = dot_nt(jnp.concatenate([ah, am], axis=0), bm)
    third = dot_nt(ah, bl)
    small = (first[2 * n:] + second[n:]) + third
    return first[:n] + ((first[n:2 * n] + second[:n]) + small)


def kernel(bt, ct_hbm, out, ring, ct, fb, e0, tb, sb, rb, lt, rl, gacc, cst, cown, gown, grecv, jt, ks, kr, kl, rsend, rrecv,
           pf, ph, dma_sem, ct_sem, fb_sem, d2d_s, d2d_r, ici_s, early_r, late_r, last_r, g_s, g_r, r_s, r_r, p_s, p_r):
    y = lax.axis_index('aux')
    o = lax.axis_index('orb')
    p = o // 2
    s = lax.rem(o, 2)
    sib = o + 1 - 2 * s
    opp = lax.rem(o + 2, 4)
    opp_sib = 3 - o
    yo = 1 - y
    keep = 2 * p
    give = 2 * (1 - p)

    def dev(yy, oo):
        return {'aux': yy, 'orb': oo}

    def remote(src, dst, ssem, rsem, to):
        return pltpu.make_async_remote_copy(src_ref=src, dst_ref=dst, send_sem=ssem, recv_sem=rsem,
                                            device_id=to, device_id_type=pl.DeviceIdType.MESH)

    def load(g, slot):
        return pltpu.make_async_copy(bt.at[pl.ds(g * GRP, GRP)], ring.at[pl.ds(slot * GRP, GRP)], dma_sem.at[lax.rem(g, 4)])

    def tail_load():
        slot = (NGRP - 1) % RING
        return pltpu.make_async_copy(bt.at[pl.ds(MAIN, TAIL)], ring.at[pl.ds(slot * GRP, TAIL)], dma_sem.at[(NGRP - 1) % 4])

    def first_load(g, h):
        lanes = pl.ds(pl.multiple_of(give * 128, 128), 128)
        rows = pl.ds(g * GRP + h * (GRP // 2), GRP // 2)
        return pltpu.make_async_copy(bt.at[rows, :, lanes], fb.at[rows], fb_sem.at[h])

    ct_copy = pltpu.make_async_copy(ct_hbm, ct, ct_sem)
    ct_copy.start()
    first_load(0, 0).start()
    first_load(0, 1).start()
    for g in range(AHEAD):
        load(g, g).start(priority=1)

    barrier = pltpu.get_barrier_semaphore()
    peers = [(y, sib), (y, opp), (y, opp_sib), (yo, o), (yo, sib), (yo, opp), (yo, opp_sib)]
    for peer in peers:
        pl.semaphore_signal(barrier, inc=1, device_id=dev(*peer), device_id_type=pl.DeviceIdType.MESH)

    t4 = tb.reshape(QT, NOCC, RPAD, 128)

    def cross(src, dst, rsem):
        return remote(src, dst, ici_s.at[0], rsem, dev(y, opp))

    def early_copy(g):
        rows = pl.ds(pl.multiple_of(g * GRP, GRP), GRP)
        return cross(t4.at[pl.ds(give, 2), :, rows], rb.at[:, :, rows], early_r)

    def early_rest(g):
        rows = pl.ds(pl.multiple_of(g * GRP, GRP), GRP)
        return cross(t4.at[pl.ds(give + 1, 1), :, rows], rb.at[pl.ds(1, 1), :, rows], early_r)

    e4 = e0.reshape(FIRST, NOCC, GRP, 128)

    def first_copy(g):
        return cross(e4.at[g], rb.at[0, :, pl.ds(g * GRP, GRP)], early_r)

    def late_copy(c):
        orbs = pl.ds(c * LATE, LATE)
        rows = pl.ds(EARLY * GRP, MAIN - EARLY * GRP)
        return cross(t4.at[pl.ds(give, 2), orbs, rows], rb.at[:, orbs, rows], late_r.at[c])

    def last_copy(c):
        rows = pl.ds(CUTS[c], SIZES[c])
        return remote(lt.at[pl.ds(give, 2), rows], rl.at[:, rows], ici_s.at[1], last_r.at[c], dev(y, opp))

    early_rows = pl.ds(0, EARLY * GRP)
    early_all = cross(t4.at[pl.ds(give, 2), :, early_rows], rb.at[:, :, early_rows], early_r)
    main_all = cross(t4.at[pl.ds(give, 2), :, pl.ds(0, MAIN)], rb, early_r)
    last_all = remote(lt.at[pl.ds(give, 2)], rl, ici_s.at[1], last_r.at[0], dev(y, opp))
    sib_all = remote(t4, sb, d2d_s, d2d_r, dev(y, sib))
    g_all = remote(grecv, grecv, g_s, g_r, dev(y, sib))

    def sib_copy(g):
        rows = pl.ds(pl.multiple_of(g * GRP, GRP), GRP)
        return remote(t4.at[:, :, rows], sb.at[:, :, rows], d2d_s, d2d_r, dev(y, sib))

    ct_copy.wait()
    c = jnp.concatenate([ct[...], jnp.zeros((2, NBF), f32)], axis=0)
    cst[...] = jnp.concatenate(pieces(c), axis=0)
    def t_rows(x):
        r = None
        for piece in pieces(x):
            term = jnp.dot(cst[...], piece, preferred_element_type=f32)
            r = term if r is None else r + term
        return r[0:32] + r[32:64] + r[64:96]

    for g in range(FIRST):
        for h in range(2):
            first_load(g, h).wait()
            if g + 1 < FIRST and h == 1:
                first_load(g + 1, 0).start()
                first_load(g + 1, 1).start()
            for j in range(h * GRP // 2, (h + 1) * GRP // 2):
                e0[pl.ds(g * NOCC * GRP + j, NOCC, stride=GRP), :] = t_rows(fb[g * GRP + j])[:NOCC]
        if g == 0:
            pl.semaphore_wait(barrier, len(peers))
        first_copy(g).start()

    mine = c[:, 0:ROWS]
    for b in range(1, 4):
        mine = jnp.where(o == b, c[:, b * ROWS:(b + 1) * ROWS], mine)
    cown[...] = jnp.concatenate([mine, jnp.zeros((32, 128 - ROWS), f32)], axis=1)
    gacc[...] = jnp.zeros_like(gacc)
    jt[...] = jnp.zeros_like(jt)
    ks[...] = jnp.zeros_like(ks)
    kr[...] = jnp.zeros_like(kr)
    kl[...] = jnp.zeros_like(kl)

    def t_group(g, rows, dense):
        slot = lax.rem(g, RING)
        if dense:
            tail_load().wait()
        else:
            @pl.when(g + AHEAD < NGRP - 1)
            def _():
                load(g + AHEAD, lax.rem(g + AHEAD, RING)).start(priority=1)

            @pl.when(g + AHEAD == NGRP - 1)
            def _():
                tail_load().start(priority=1)
            load(g, slot).wait()
        cg = pltpu.roll(cown[...], lax.rem(128 - g * GRP, 128), 1)
        for j in range(rows):
            m = g * GRP + j
            t = t_rows(ring[slot * GRP + j])
            gacc[:, 0:NQ] += t * cg[:, j:j + 1]
            for k in range(QT):
                hi = min(NQ, 128 * (k + 1))
                tt = t[:NOCC, 128 * k:hi]
                if hi < 128 * (k + 1):
                    tt = jnp.concatenate([tt, jnp.zeros((NOCC, 128 * (k + 1) - hi), f32)], axis=1)
                tb[k, pl.ds(m, NOCC, stride=RPAD), :] = tt
                if dense:
                    lt[k, pl.ds(j, NOCC, stride=TAIL), :] = tt
        sib_copy(g).start()

    def t_step(g, carry):
        t_group(g, GRP, False)

        @pl.when(g < FIRST)
        def _():
            early_rest(g).start()

        @pl.when((g >= FIRST) & (g < EARLY))
        def _():
            early_copy(g).start()
        return carry

    lax.fori_loop(0, NGRP - 1, t_step, 0)
    for k in range(QT):
        tb[k, pl.ds(ROWS, NOCC, stride=RPAD), :] = jnp.zeros((NOCC, 128), f32)
        lt[k, DENSE - GRP:, :] = jnp.zeros((GRP, 128), f32)
    t_group(NGRP - 1, TAIL, True)

    gown[...] = jnp.sum(gacc[...], axis=0, keepdims=True)
    g_copies = [remote(gown, grecv.at[k], g_s, g_r, dev(y, to))
                for k, to in enumerate((sib, opp, opp_sib))]
    for copy in g_copies:
        copy.start()

    def late_start(c, carry):
        late_copy(c).start()
        return carry

    lax.fori_loop(0, NOCC // LATE, late_start, 0)

    for c in range(len(CUTS) - 1):
        last_copy(c).start()

    sib_all.wait_recv()

    def both(tiles_own, tiles_sib):
        own = jnp.concatenate(tiles_own, axis=1)
        other = jnp.concatenate(tiles_sib, axis=1)
        gap = jnp.zeros((128 - RPAD, own.shape[1]), f32)
        return own, jnp.concatenate([own, gap, other], axis=0)

    def k_self(i):
        own, stack = both([t4[k, i] for k in range(QT)], [sb[k, i] for k in range(QT)])
        res = full_nt(own, stack)
        ks[:, 0:128 + RPAD] += res

    def self_step(i, carry):
        k_self(i)
        return carry

    ahead = NOCC - 2 * NGRP
    lax.fori_loop(0, ahead, self_step, 0)

    g_all.wait()
    gam = gown[...] + grecv[0] + grecv[1] + grecv[2]
    gown[...] = gam
    lane = lax.broadcasted_iota(jnp.int32, (NBF, 128), 1)

    def j_step(n, carry):
        g = lax.rem(n + AGAIN, NGRP)
        slot = lax.rem(n + AGAIN, RING)

        @pl.when((n >= 1) & (n <= AGAIN))
        def _():
            load(n - 1, lax.rem(n - 1 + AGAIN, RING)).start(priority=1)

        @pl.when(n >= RING)
        def _():
            load(g, slot).wait()
        gv = gown[:, 0:NQ]
        acc = jt[...]
        for j in range(GRP):
            x = ring[slot * GRP + j]
            col = jnp.sum(x * gv, axis=1, keepdims=True)
            acc = jnp.where(lane == g * GRP + j, col, acc)
        jt[...] = acc
        k_self(ahead + 2 * n)
        k_self(ahead + 2 * n + 1)
        return carry

    lax.fori_loop(0, NGRP, j_step, 0)

    lane88 = lax.broadcasted_iota(jnp.int32, (RPAD, 128), 1)

    def columns(first, second):
        a = jnp.where(s == 0, first, second)
        b = pltpu.roll(jnp.where(s == 0, second, first), ROWS, 1)
        return jnp.concatenate([jnp.where(lane88 < ROWS, a, b), b], axis=1)[:, 0:HALF]

    jrows = jnp.transpose(jt[...])[0:RPAD]
    j0 = 2.0 * jrows[:, 0:HALF]
    j1 = 2.0 * jrows[:, HALF:2 * HALF]
    kself = columns(ks[:, 0:128], ks[:, 128:256])
    h0 = j0 - jnp.where(p == 0, kself, 0.0)
    h1 = j1 - jnp.where(p == 1, kself, 0.0)
    rsend[:, 0:HALF] = jnp.where(y == 0, h1, h0)
    base = jnp.where(y == 0, h0, h1)
    ks[:, 0:HALF] = base
    r_copy = remote(rsend, rrecv, r_s, r_r, dev(yo, o))
    r_copy.start()

    early_all.wait_recv()

    def k_cross(i, moved):
        _, stack = both([t4[keep + k, i] for k in range(2)], [sb[keep + k, i] for k in range(2)])
        return full_nt(jnp.concatenate(moved, axis=1), stack)

    def r_step(c, carry):
        @pl.when(lax.rem(c, LATE // ICH) == 0)
        def _():
            late_copy(c // (LATE // ICH)).wait_recv()
        for di in range(ICH):
            i = c * ICH + di
            kr[:, 0:128 + RPAD] += k_cross(i, [rb[k, i, 0:MAIN] for k in range(2)])
        return carry

    lax.fori_loop(0, NCH, r_step, 0)

    def sends(src, lo, n, base):
        rows = pl.ds(lo, n)
        left, right = pl.ds(0, 128), pl.ds(128, 128)
        full_s, half_s = p_s.at[0], p_s.at[1]
        full_r, half_r = p_r.at[base], p_r.at[base + 1]
        return (remote(src, pf.at[0, rows], full_s, full_r, dev(y, opp)),
                remote(src, pf.at[1, rows], full_s, full_r, dev(yo, opp)),
                remote(src.at[:, left], ph.at[0, rows], half_s, half_r, dev(yo, o)),
                remote(src.at[:, right], ph.at[1, rows], half_s, half_r, dev(y, sib)),
                remote(src.at[:, right], ph.at[2, rows], half_s, half_r, dev(yo, sib)),
                remote(pf.at[:, rows], pf.at[:, rows], full_s, full_r, dev(y, opp)),
                remote(ph.at[:, rows], ph.at[:, rows], half_s, half_r, dev(y, sib)),
                remote(ph.at[pl.ds(0, 2), rows], ph.at[pl.ds(0, 2), rows], half_s, half_r, dev(y, sib)))

    main = sends(kr, 0, MAIN, 0)
    last = sends(kl, MAIN, GRP, 2)
    whole = sends(rsend, 0, RPAD, 0)

    @pl.when(y == p)
    def _():
        for k in (0, 4, 2):
            main[k].start()

    @pl.when(y != p)
    def _():
        main[1].start()
        main[3].start()

    sib_all.wait_send()
    main_all.wait_send()
    r_copy.wait()
    done = ks[:, 0:HALF] + rrecv[:, 0:HALF]
    ks[:, 0:HALF] = done

    @pl.when(y == p)
    def _():
        out[...] = done[0:ROWS]

    def last_step(n, carry):
        for c, first in enumerate(SENDS[:-1]):
            @pl.when(n == first // LSTEP)
            def _():
                last_copy(c).wait_recv()
        gap = jnp.zeros((GRP - TAIL, 128), f32)
        own, other, moved = [], [], []
        for di in range(LSTEP):
            i = n * LSTEP + di
            for k in range(2):
                own.append(t4[keep + k, i])
                other.append(sb[keep + k, i])
                moved.append(jnp.concatenate([rl[k, pl.ds(TAIL * i, TAIL), :], gap], axis=0))
        moved = jnp.concatenate(moved, axis=1)
        kl[:, 0:RPAD] += full_nt(moved, jnp.concatenate(own, axis=1))
        kl[:, 128:128 + RPAD] += full_nt(moved, jnp.concatenate(other, axis=1))
        return carry

    lax.fori_loop(0, NOCC // LSTEP, last_step, 0)

    def sent():
        last_all.wait_send()

    @pl.when(y == p)
    def _():
        for k in (0, 4, 2):
            last[k].start()
        sent()
        whole[0].wait_send()
        whole[7].wait_send()

    @pl.when(y != p)
    def _():
        last[1].start()
        last[3].start()
        sent()

        def turn(x):
            return jnp.transpose(jnp.concatenate([x, jnp.zeros((40, 128), f32)], axis=0))[0:RPAD]

        main[6].wait_recv()
        main[5].wait_recv()
        last[6].wait_recv()
        mine_opp = jnp.concatenate([kr[:, 0:128], kl[:, 0:128]], axis=0)
        col_opp = turn(mine_opp + ph[0])
        col_sib = turn(ph[1] + ph[2])
        last[5].wait_recv()
        block_a = (pf[0, :, 0:128] + pf[1, :, 0:128]) + col_opp
        block_b = (pf[0, :, 128:256] + pf[1, :, 128:256]) + col_sib
        res = ks[:, 0:HALF] - columns(block_a, block_b)
        out[...] = res[0:ROWS]
        whole[0].wait_send()
        whole[3].wait_send()


def solution(mesh):
    sem = pltpu.SemaphoreType.DMA

    def local_fock(fit_loc, orbitals):
        bt = jnp.transpose(fit_loc, (1, 2, 0))
        ct = jnp.transpose(orbitals)
        return pl.pallas_call(
            kernel,
            out_shape=pltpu.VMEM((ROWS, HALF), f32),
            in_specs=[pl.BlockSpec(memory_space=pl.ANY), pl.BlockSpec(memory_space=pl.ANY)],
            out_specs=pl.BlockSpec(memory_space=pltpu.VMEM),
            scratch_shapes=[
                pltpu.VMEM((RING * GRP, NBF, NQ), f32),
                pltpu.VMEM((NOCC, NBF), f32),
                pltpu.VMEM((FIRST * GRP, NBF, 128), f32),
                pltpu.VMEM((FIRST * NOCC * GRP, 128), f32),
                pltpu.VMEM((QT, NOCC * RPAD, 128), f32),
                pltpu.VMEM((QT, NOCC, RPAD, 128), f32),
                pltpu.VMEM((2, NOCC, MAIN, 128), f32),
                pltpu.VMEM((QT, DENSE, 128), f32),
                pltpu.VMEM((2, DENSE, 128), f32),
                pltpu.VMEM((32, 512), f32),
                pltpu.VMEM((96, NBF), bf16),
                pltpu.VMEM((32, 128), f32),
                pltpu.VMEM((1, 512), f32),
                pltpu.VMEM((3, 1, 512), f32),
                pltpu.VMEM((NBF, 128), f32),
                pltpu.VMEM((RPAD, 256), f32),
                pltpu.VMEM((MAIN, 256), f32),
                pltpu.VMEM((GRP, 256), f32),
                pltpu.VMEM((RPAD, 256), f32),
                pltpu.VMEM((RPAD, 256), f32),
                pltpu.VMEM((2, RPAD, 256), f32),
                pltpu.VMEM((3, RPAD, 128), f32),
                sem((4,)), sem, sem((2,)), sem, sem, sem((2,)), sem, sem((NOCC // LATE,)), sem((len(CUTS) - 1,)),
                sem, sem, sem, sem, sem((2,)), sem((4,)),
            ],
            compiler_params=pltpu.CompilerParams(collective_id=0, has_side_effects=True,
                                                 vmem_limit_bytes=63 << 20),
            name='fock',
        )(bt, ct)

    spec_fit = P(('sys', 'aux'), 'orb', None)
    spec_orbitals = P('sys', None)
    spec_out = P(('sys', 'orb'), 'aux')
    return jax.shard_map(local_fock, mesh=mesh, in_specs=(spec_fit, spec_orbitals), out_specs=spec_out, check_vma=False)
```
